1024 devices in a mesh: grp: 64 (over y_lo, z, core), blk: 16 (over y_hi, x).
Axes of the slice: x: 8, y: 8 (y_hi: 2, y_lo: 4; y = y_hi * 4 + y_lo), z: 8, core: 2. Of those that a mesh axis runs over, the one named last changes fastest.
Arguments:
- integrals: bfloat16 [8, 128, 128, 128], P(None, 'blk'), may hold values from -0.5 to 0.5
- doubles: bfloat16 [64, 128, 128], P('blk'), may hold values from -0.0059814453 to 0.0059814453
- coulomb: bfloat16 [64, 128, 128], P('blk'), may hold values from -0.1796875 to 0.1796875
- singles: float32 [8, 128], P(None, 'blk'), may hold values from -0.18 to 0.18
- occ_energy: float32 [8], replicated, may hold values from -2 to -0.5
- vir_energy: float32 [128], replicated, may hold values from 0.3 to 3
- triplets: int32 [64, 16, 3], P('grp'), may hold values from 0 to 7
- tile_count: int32 [64], P('grp'), may hold values from 1 to 16, as said below
Outputs:
- triplet_energy: float32 [64, 16], P('grp')
- mean_energy: float32 [], replicated
The draws below stay inside these ranges and needn't reach their ends.
Inputs may be any that keep to these rules, and one draw needn't show every extreme that they name: `tile_count`: slots with an index below a group's count are live; some group has all 16 slots live.
All inputs are finite; a program needn't handle non-finite values.
Results may differ from the reference program's by a relative error of at most 0.0003.
Values may be sent and summed in bfloat16 or wider, within the bound.
No kernel may reach another device: no remote copies, remote signals or barrier semaphores. Data moves between devices by JAX's collectives and lax.ppermute only.
A program may use at most 64 MiB of HBM per device.

```python
import jax
import jax.numpy as jnp
from jax import lax

NO = 8
NV = 128
TRIP = 16
GROUPS = 64


def draw_tile_count(key, part):
    key_counts = jax.random.fold_in(key, 11)
    key_full = jax.random.fold_in(key, 12)
    counts = jax.random.randint(key_counts, (GROUPS,), max(1, TRIP // 4), TRIP + 1)
    fullest = jax.random.randint(key_full, (), 0, GROUPS)
    return jnp.where(jnp.arange(GROUPS) == fullest, TRIP, counts).astype(jnp.int32)


def with_ends(drawn, rng, least, top_value):
    place = [jax.random.randint(jax.random.fold_in(rng, axis), (), 0, length) for axis, length in enumerate(drawn.shape)]
    main_axis = drawn.shape.index(max(drawn.shape))
    beside = place[:main_axis] + [(place[main_axis] + 1) % drawn.shape[main_axis]] + place[main_axis + 1:]
    return drawn.at[tuple(place)].set(least).at[tuple(beside)].set(top_value)


def level_of(stream_key, extent, split, smallest, high):
    factor_of = 1.0
    for dim, shards_of in split:
        draws = jax.random.uniform(jax.random.fold_in(jax.random.fold_in(stream_key, 6), dim), (shards_of,), jnp.float32, smallest / len(split), high / len(split))
        factor_of = factor_of * jnp.repeat(jnp.exp(draws), extent[dim] // shards_of).reshape((-1,) + (1,) * (len(extent) - 1 - dim))
    return factor_of


def gaussian(own_key, shape, deviation, bound, split=(), kind=jnp.bfloat16):
    entries = jax.random.normal(own_key, shape, jnp.float32) * deviation
    if len(split) > 0:
        entries = level_of(own_key, shape, split, -0.22, 0.18) * entries
    return jnp.clip(entries, min=-bound, max=bound).astype(kind)


def setup_inputs(seed: int = 0) -> dict:
    streams_of = jax.random.split(jax.random.key(seed), 9)
    integrals = gaussian(streams_of[0], (NO, NV, NV, NV), NV ** -0.5, 0.5, ((1, 16),))
    doubles = gaussian(streams_of[1], (NO * NO, NV, NV), 0.001, 0.0059814453, ((0, 16),))
    coulomb = gaussian(streams_of[2], (NO * NO, NV, NV), 0.03, 0.1796875, ((0, 16),))
    singles = gaussian(streams_of[3], (NO, NV), 0.03, 0.18, ((1, 16),), jnp.float32)
    occ_energy = jnp.clip(jax.random.uniform(streams_of[4], (NO,), jnp.float32, -2.0, -0.5), -2.0, -0.5)
    vir_energy = jnp.clip(jax.random.uniform(streams_of[5], (NV,), jnp.float32, 0.3, 3.0), 0.3, 3.0)
    triplets = with_ends(jax.random.randint(streams_of[6], (GROUPS, TRIP, 3), 0, NO), jax.random.fold_in(streams_of[6], 1), 0, NO - 1).astype(jnp.int32)
    tile_count = draw_tile_count(jax.random.fold_in(streams_of[8], 71), 0)
    return dict(integrals=integrals, doubles=doubles, coulomb=coulomb, singles=singles, occ_energy=occ_energy, vir_energy=vir_energy, triplets=triplets, tile_count=tile_count)


def slot_energy(integrals, doubles, coulomb, singles, occ_energy, vir_energy, triplet):
    first_occ = triplet[0]
    second_occ = triplet[1]
    third_occ = triplet[2]
    slab_rows = integrals[first_occ].reshape(NV * NV, NV)
    doubles_kj = doubles[third_occ * NO + second_occ]
    doubles_jk = doubles[second_occ * NO + third_occ]
    first = jnp.dot(slab_rows, doubles_kj.T, preferred_element_type=jnp.float32).reshape(NV, NV, NV)
    second = jnp.dot(slab_rows, doubles_jk.T, preferred_element_type=jnp.float32).reshape(NV, NV, NV)
    connected = first + jnp.transpose(second, (0, 2, 1))
    coupling = coulomb[second_occ * NO + third_occ].astype(jnp.float32)
    full = connected + singles[first_occ][:, None, None] * coupling[None, :, :]
    occ_sum = occ_energy[first_occ] + occ_energy[second_occ] + occ_energy[third_occ]
    denominator = occ_sum - vir_energy[:, None, None] - vir_energy[None, :, None] - vir_energy[None, None, :]
    return jnp.sum(full * full / denominator)


def reference(integrals, doubles, coulomb, singles, occ_energy, vir_energy, triplets, tile_count):
    flat_triplets = triplets.reshape(GROUPS * TRIP, 3)

    def one_slot(triplet):
        return slot_energy(integrals, doubles, coulomb, singles, occ_energy, vir_energy, triplet)

    energies = lax.map(one_slot, flat_triplets).reshape(GROUPS, TRIP)
    slot_ids = jnp.arange(TRIP, dtype=jnp.int32)
    live = slot_ids[None, :] < tile_count[:, None]
    triplet_energy = jnp.where(live, energies, jnp.zeros_like(energies))
    mean_energy = jnp.sum(triplet_energy) / (GROUPS * TRIP)
    return triplet_energy, mean_energy
```

```python
import functools

import jax
import jax.numpy as jnp
import numpy as np
from jax import lax
from jax.experimental import pallas as pl
from jax.experimental.pallas import tpu as pltpu
from jax.sharding import Mesh
from jax.sharding import PartitionSpec as P

AXES = ("yl", "z", "c", "yh", "x")
SIZES = (4, 8, 2, 2, 8)
GRP = ("yl", "z", "c")
BLK = ("yh", "x")
PLANE = ("yh", "yl", "x")
STACK = ("z", "c")
NO = 8
SMALL = pltpu.CompilerParams(vmem_limit_bytes=8 * 1024 * 1024)


def device_at(yl, z, c, yh, x):
    return ((((yl * 8) + z) * 2 + c) * 2 + yh) * 8 + x


def pair_of(yl, z, c, yh, x):
    row_yh = yh ^ c
    row_x = (x - z - 4 * c) & 7
    second = row_yh * 4 + (row_x >> 1)
    third = (row_x & 1) * 4 + ((row_x >> 1) ^ yl) % 4
    return row_yh, row_x, second, third


def routes():
    straight, swapped = [], []
    for yl, z, c, yh, x in np.ndindex(*SIZES):
        row_yh, row_x, second, third = pair_of(yl, z, c, yh, x)
        here = device_at(yl, z, c, yh, x)
        from_yl = yl ^ (2 * int(row_yh != yh))
        straight.append((device_at(from_yl, z, c, row_yh, row_x), here))
        owner = third * 2 + second // 4
        from_yl = yl ^ (2 * int(owner // 8 != yh))
        swapped.append((device_at(from_yl, z, c, owner // 8, owner % 8), here))
    return straight, swapped


def recip_kernel(shift_ref, sums_ref, out_ref):
    sums = sums_ref[...]

    def one_row(r, carry):
        out_ref[pl.ds(r, 1)] = 1.0 / (shift_ref[pl.ds(r, 1), :] - sums)[None]
        return carry

    lax.fori_loop(0, out_ref.shape[0], one_row, 0, unroll=2)


def energy_kernel(ints_ref, rows_ref, swap_ref, recip_ref, amps_ref, info_ref, out_ref, sums_ref):
    occupied, width_block, width, _ = ints_ref.shape
    block_jk = rows_ref[0]
    coupling = rows_ref[1].astype(jnp.float32)
    block_kj = swap_ref[...]
    contract = (((1,), (1,)), ((), ()))

    def one_occ(i, carry):
        total = jnp.zeros((8, width), jnp.float32)
        for a in range(width_block):
            slab = ints_ref[i, a]
            left = jnp.concatenate([slab, block_jk], axis=1)
            right = jnp.concatenate([block_kj, slab], axis=1)
            connected = lax.dot_general(left, right, contract, preferred_element_type=jnp.float32)
            amp = amps_ref[pl.ds(i * width_block + a, 1), :]
            full = connected + amp * coupling
            value = full * full * recip_ref[i * width_block + a]
            total = total + jnp.sum(value.reshape(width // 8, 8, width), axis=0)
        sums_ref[pl.ds(i, 1), :] = jnp.sum(total, axis=0, keepdims=True)
        return carry

    lax.fori_loop(0, occupied, one_occ, 0)
    energies = jnp.sum(sums_ref[...], axis=1, keepdims=True)
    sub = lax.broadcasted_iota(jnp.int32, (occupied, 128), 0)
    lane = lax.broadcasted_iota(jnp.int32, (occupied, 128), 1)
    row = jnp.sum(jnp.where(sub == lane, energies, 0.0), axis=0, keepdims=True)
    out_ref[...] = jnp.broadcast_to(row + info_ref[...], out_ref.shape)


def table_kernel(in_ref, out_ref):
    got = in_ref[...]
    lane = lax.broadcasted_iota(jnp.int32, got.shape, 1).astype(jnp.float32)
    pick = jnp.where(lane < 64.0, got[:, 16:17], got[:, 17:18] + 64.0) == lane
    both = lax.dot_general(
        got,
        pick.astype(jnp.float32),
        (((0,), (0,)), ((), ())),
        precision=lax.Precision.HIGHEST,
        preferred_element_type=jnp.float32,
    )
    low = lax.broadcasted_iota(jnp.int32, (8, 128), 1) < 64
    packed = jnp.where(low, both[0:8], both[8:16])
    peers = out_ref.shape[0] // 8
    out_ref[...] = jnp.broadcast_to(packed[None], (peers, 8, 128)).reshape(peers * 8, 128)


def final_kernel(in_ref, first_ref, pair_ref, trip_ref, mean_ref):
    peers = in_ref.shape[0] // 8
    table = jnp.sum(in_ref[...].reshape(peers, 8, 128), axis=0)
    counts = pltpu.roll(table, 64, 1)
    low = lax.broadcasted_iota(jnp.int32, (8, 128), 1) < 64
    weighted = jnp.where(low, table * counts, 0.0)
    mean_ref[...] = jnp.sum(jnp.sum(weighted, axis=0, keepdims=True), axis=1, keepdims=True) / 1024.0
    chosen = jnp.zeros((16, 128), jnp.float32)
    for i in range(8):
        chosen = chosen + first_ref[:, i:i + 1] * table[i:i + 1, :]
    values = jnp.sum(chosen * pair_ref[...], axis=1, keepdims=True)
    sub = lax.broadcasted_iota(jnp.int32, (16, 128), 0)
    lane = lax.broadcasted_iota(jnp.int32, (16, 128), 1)
    row = jnp.sum(jnp.where(sub == lane, values, 0.0), axis=0, keepdims=True)
    trip_ref[...] = row[:, :16]


def vmem(count):
    return [pl.BlockSpec(memory_space=pltpu.VMEM)] * count


def kept(*arrays):
    return [pltpu.with_memory_space_constraint(a, pltpu.VMEM) for a in arrays]


def body(integrals, doubles, coulomb, singles, occ_energy, vir_energy, triplets, tile_count):
    occupied, width_block, width, _ = integrals.shape
    slots = triplets.shape[1]
    yl, z, c, yh, x = (lax.axis_index(axis) for axis in AXES)
    place = yh * 8 + x
    straight, swapped = routes()

    low_bits = (place >> 1) & 3
    target_yl = yl ^ (2 * c)
    swap_yl = yl ^ (2 * (yh ^ (x & 1) ^ c))
    row_straight = low_bits ^ target_yl
    row_swapped = low_bits ^ swap_yl
    take = functools.partial(lax.dynamic_index_in_dim, axis=0, keepdims=False)
    sent = jnp.stack([take(doubles, row_straight), take(coulomb, row_straight)])
    rows = lax.ppermute(sent, AXES, straight)
    swap = lax.ppermute(take(doubles, row_swapped), AXES, swapped)

    _, _, second, third = pair_of(yl, z, c, yh, x)
    own_pair = second * NO + third
    vir_block = lax.dynamic_slice_in_dim(vir_energy, place * width_block, width_block)
    occ_sums = occ_energy + occ_energy[second] + occ_energy[third]
    shifts = (occ_sums[:, None] - vir_block[None, :]).reshape(-1)
    vir_sums = vir_energy[:, None] + vir_energy[None, :]
    shifts = jnp.broadcast_to(shifts[:, None], (occupied * width_block, width))
    recip = pl.pallas_call(
        recip_kernel,
        out_shape=pltpu.VMEM((occupied * width_block, width, width), jnp.float32),
        in_specs=vmem(2),
        out_specs=vmem(1)[0],
        compiler_params=SMALL,
        name="reciprocals",
    )(*kept(shifts, vir_sums))
    amps = jnp.broadcast_to(singles.reshape(-1, 1), (occupied * width_block, width))

    lane = jnp.arange(128, dtype=jnp.int32)
    live = jnp.arange(slots, dtype=jnp.int32) < tile_count[0]
    firsts = triplets[0, :, 0]
    pairs = triplets[0, :, 1] * NO + triplets[0, :, 2]
    first_hot = ((firsts[:, None] == lane[None, :]) & live[:, None]).astype(jnp.float32)
    pair_hot = (pairs[:, None] == lane[None, :]).astype(jnp.float32)
    my_first = firsts[place]
    my_pair = pairs[place]
    my_live = place < tile_count[0]
    info = jnp.where((lane == my_first + 8) & my_live, 1.0, 0.0)
    info = jnp.where(lane == 16, own_pair.astype(jnp.float32), info)
    info = jnp.where(lane == 17, my_pair.astype(jnp.float32), info)

    recip, amps, info, first_hot, pair_hot = lax.optimization_barrier((recip, amps, info, first_hot, pair_hot))
    message = pl.pallas_call(
        energy_kernel,
        out_shape=pltpu.VMEM((64, 128), jnp.float32),
        in_specs=vmem(6),
        out_specs=vmem(1)[0],
        scratch_shapes=[pltpu.VMEM((occupied, width), jnp.float32)],
        compiler_params=SMALL,
        name="energies",
    )(*kept(integrals, rows, swap, recip, amps, info[None]))
    message = lax.all_to_all(message, PLANE, 0, 0, tiled=True)
    tables = pl.pallas_call(
        table_kernel,
        out_shape=pltpu.VMEM((128, 128), jnp.float32),
        in_specs=vmem(1),
        out_specs=vmem(1)[0],
        compiler_params=SMALL,
        name="table",
    )(*kept(message))
    tables = lax.all_to_all(tables, STACK, 0, 0, tiled=True)
    trip, mean = pl.pallas_call(
        final_kernel,
        out_shape=(
            jax.ShapeDtypeStruct((1, slots), jnp.float32),
            jax.ShapeDtypeStruct((1, 1), jnp.float32),
        ),
        in_specs=vmem(3),
        out_specs=tuple(vmem(2)),
        compiler_params=SMALL,
        name="lookup",
    )(*kept(tables, first_hot, pair_hot))
    return trip, mean.reshape(())


def solution(mesh):
    fine = Mesh(mesh.devices.reshape(SIZES), AXES)
    in_specs = (
        P(None, BLK, None, None),
        P(BLK, None, None),
        P(BLK, None, None),
        P(None, BLK),
        P(),
        P(),
        P(GRP, None, None),
        P(GRP),
    )
    out_specs = (P(GRP, None), P())
    return jax.shard_map(body, mesh=fine, in_specs=in_specs, out_specs=out_specs, check_vma=False)
```

```python
import jax
import jax.numpy as jnp
import numpy as np
from jax import lax
from jax.experimental import pallas as pl
from jax.experimental.pallas import tpu as pltpu
from jax.sharding import Mesh
from jax.sharding import PartitionSpec as P

AXES = ("yl", "z", "c", "yh", "x")
SIZES = (4, 8, 2, 2, 8)
GRP = ("yl", "z", "c")
BLK = ("yh", "x")
PLANE = ("yh", "yl", "x")
STACK = ("z", "c")
NO = 8
WORKERS = 4
SMALL = pltpu.CompilerParams(vmem_limit_bytes=12 * 1024 * 1024)
F32 = jnp.float32


def device_at(yl, z, c, yh, x):
    return ((((yl * 8) + z) * 2 + c) * 2 + yh) * 8 + x


def owners_of(yl, z, c, yh, x):
    low, high = z & 1, z >> 1 & 1
    none, one, more = yl == 0, yl == 1, yl > 1
    offset = none * (low + 2 * high + 4 * c) + one * (low + 4 * high + 8 * c) + more * (low + 2 * high + 8 * c)
    owner = (yh * 8 + x) ^ offset
    swapped = (owner & 1) << 3 | (owner & 6) ^ (yl << 1) | owner >> 3
    return owner, none * (owner ^ 9) + (1 - none) * swapped


def pair_at(owner, yl):
    return owner >> 1, (owner & 1) * 4 + ((owner >> 1 & 3) ^ yl)


def routes():
    first, second = [], []
    for yl, z, c, yh, x in np.ndindex(*SIZES):
        if z < WORKERS:
            here = device_at(yl, z, c, yh, x)
            for route, owner in zip((first, second), owners_of(yl, z, c, yh, x)):
                route.append((device_at(yl, z, c, owner >> 3, owner & 7), here))
    return first, second


def where_am_i():
    yl, z, c, yh, x = (lax.axis_index(axis) for axis in AXES)
    return yl, z, c, yh, x


def own_pairs():
    yl, z, c, yh, x = where_am_i()
    none = (yl == 0).astype(jnp.int32)
    one = (yl == 1).astype(jnp.int32)
    more = (yl > 1).astype(jnp.int32)
    low, high = z & 1, (z >> 1) & 1
    offset = none * (low + 2 * high + 4 * c) + one * (low + 4 * high + 8 * c) + more * (low + 2 * high + 8 * c)
    owner = (yh * 8 + x) ^ offset
    swapped = ((owner & 1) << 3) | ((owner & 6) ^ (yl << 1)) | (owner >> 3)
    other = none * (owner ^ 9) + (1 - none) * swapped
    return pair_at(owner, yl), pair_at(other, yl)


def rows_kernel(doubles_ref, coulomb_ref, out_ref, sems):
    yl, _, _, yh, x = where_am_i()
    row = (((yh * 8 + x) >> 1) & 3) ^ yl
    copies = [
        pltpu.make_async_copy(doubles_ref.at[row], out_ref.at[0], sems.at[0]),
        pltpu.make_async_copy(coulomb_ref.at[row], out_ref.at[1], sems.at[1]),
    ]
    for copy in copies:
        copy.start()
    for copy in copies:
        copy.wait()


def prep_kernel(ints_ref, trip_ref, count_ref, occ_ref, vir_ref, singles_ref, virs_ref,
                slab_ref, recip_ref, amps_ref, info_ref, first_ref, pair_ref, sem):
    occupied, width_block = singles_ref.shape
    width = virs_ref.shape[1]
    slots = first_ref.shape[0]
    _, z, _, yh, x = where_am_i()
    place = yh * 8 + x
    (j1, k1), (j2, k2) = own_pairs()
    diagonal = j1 == k1
    busy = z < WORKERS
    live = count_ref[0]
    slabs = pltpu.make_async_copy(ints_ref, slab_ref, sem)

    @pl.when(busy)
    def _():
        slabs.start()

    lane = lax.broadcasted_iota(jnp.int32, (1, 128), 1)
    mine = jnp.where(place < live, trip_ref[0, 0, place] + 16, -1)
    info = jnp.where(lane == mine, 1.0, 0.0)
    info = jnp.where(lane == 24, jnp.where(busy, j1 * NO + k1, -1).astype(F32), info)
    info = jnp.where(lane == 25, jnp.where(busy, j2 * NO + k2, -1).astype(F32), info)
    info = jnp.where(lane == 26, (trip_ref[1, 0, place] * NO + trip_ref[2, 0, place]).astype(F32), info)
    info_ref[...] = info

    sub = lax.broadcasted_iota(jnp.int32, (slots, 128), 0)
    lanes = lax.broadcasted_iota(jnp.int32, (slots, 128), 1)
    first_at = jnp.full((slots, 128), -1, jnp.int32)
    pair_at_ = jnp.full((slots, 128), -1, jnp.int32)
    for s in range(slots):
        first_at = jnp.where(sub == s, jnp.where(s < live, trip_ref[0, 0, s], -1), first_at)
        pair_at_ = jnp.where(sub == s, trip_ref[1, 0, s] * NO + trip_ref[2, 0, s], pair_at_)
    first_ref[...] = jnp.where(first_at == lanes, 1.0, 0.0)
    pair_ref[...] = jnp.where(pair_at_ == lanes, 1.0, 0.0)

    def fill(table, second, third, write_amps):
        across = jnp.broadcast_to(virs_ref[...], (width, width))
        sums = across.T + across

        def one_occ(i, carry):
            occ_sum = occ_ref[i] + occ_ref[second] + occ_ref[third]
            for a in range(width_block):
                r = i * width_block + a
                recip_ref[table, r] = 1.0 / ((occ_sum - vir_ref[place * width_block + a]) - sums)
                if write_amps:
                    amps_ref[pl.ds(r, 1), :] = jnp.full((1, 128), singles_ref[i, a], F32)
            return carry

        lax.fori_loop(0, occupied, one_occ, 0)

    @pl.when(busy)
    def _():
        fill(0, j1, k1, True)

    @pl.when(jnp.logical_and(busy, diagonal))
    def _():
        fill(1, j2, k2, False)

    @pl.when(busy)
    def _():
        slabs.wait()


def energy_kernel(ints_ref, one_ref, two_ref, recip_ref, amps_ref, info_ref, out_ref, sums_ref):
    occupied, width_block, width, _ = ints_ref.shape
    _, z, _, _, _ = where_am_i()
    (j1, k1), _ = own_pairs()
    diagonal = j1 == k1
    sums_ref[...] = jnp.zeros(sums_ref.shape, F32)

    def fold(value):
        return jnp.sum(value.reshape(width // 8, 8, width), axis=0)

    def both(couple):
        amps = jnp.concatenate([one_ref[0], two_ref[0]], axis=0)
        coupling_one = one_ref[1].astype(F32)
        coupling_two = two_ref[1].astype(F32)
        if couple:
            coupling_two = coupling_two.T

        def one_occ(i, carry):
            slab = ints_ref[i].reshape(width_block * width, width)
            products = lax.dot_general(slab, amps, (((1,), (1,)), ((), ())), preferred_element_type=F32)
            total_one = jnp.zeros((8, width), F32)
            total_two = jnp.zeros((8, width), F32)
            for a in range(width_block):
                r = i * width_block + a
                left = products[a * width:(a + 1) * width, :width]
                right = products[a * width:(a + 1) * width, width:]
                amp = amps_ref[pl.ds(r, 1), :]
                recip_one = recip_ref[0, r]
                if couple:
                    connected_one = right + left.T
                    connected_two = connected_one
                    recip_two = recip_one
                else:
                    connected_one = left + left.T
                    connected_two = right + right.T
                    recip_two = recip_ref[1, r]
                full_one = connected_one + amp * coupling_one
                full_two = connected_two + amp * coupling_two
                total_one = total_one + fold(full_one * full_one * recip_one)
                total_two = total_two + fold(full_two * full_two * recip_two)
            sums_ref[pl.ds(i, 1), :] = jnp.sum(total_one, axis=0, keepdims=True)
            sums_ref[pl.ds(i + occupied, 1), :] = jnp.sum(total_two, axis=0, keepdims=True)
            return carry

        lax.fori_loop(0, occupied, one_occ, 0)

    busy = z < WORKERS

    @pl.when(jnp.logical_and(busy, jnp.logical_not(diagonal)))
    def _():
        both(True)

    @pl.when(jnp.logical_and(busy, diagonal))
    def _():
        both(False)

    energies = jnp.sum(sums_ref[...], axis=1, keepdims=True)
    sub = lax.broadcasted_iota(jnp.int32, (2 * occupied, 128), 0)
    lane = lax.broadcasted_iota(jnp.int32, (2 * occupied, 128), 1)
    row = jnp.sum(jnp.where(sub == lane, energies, 0.0), axis=0, keepdims=True)
    out_ref[...] = jnp.broadcast_to(row + info_ref[...], out_ref.shape)


def table_kernel(in_ref, out_ref):
    got = in_ref[...]
    lane = lax.broadcasted_iota(jnp.int32, got.shape, 1)
    lane_at = lane.astype(F32)
    lists = got[:, 26:27] + 64.0

    def gathered(pick):
        return lax.dot_general(
            got,
            (pick == lane_at).astype(F32),
            (((0,), (0,)), ((), ())),
            precision=lax.Precision.HIGHEST,
            preferred_element_type=F32,
        )

    ones = gathered(jnp.where(lane < 64, got[:, 24:25], lists))
    twos = gathered(got[:, 25:26])
    low = lax.broadcasted_iota(jnp.int32, (8, 128), 1) < 64
    packed = jnp.where(low, ones[0:8] + twos[8:16], ones[16:24])
    peers = out_ref.shape[0] // 8
    out_ref[...] = jnp.broadcast_to(packed[None], (peers, 8, 128)).reshape(peers * 8, 128)


def final_kernel(in_ref, first_ref, pair_ref, trip_ref, mean_ref):
    peers = in_ref.shape[0] // 8
    table = jnp.sum(in_ref[...].reshape(peers, 8, 128), axis=0)
    counts = pltpu.roll(table, 64, 1)
    low = lax.broadcasted_iota(jnp.int32, (8, 128), 1) < 64
    weighted = jnp.where(low, table * counts, 0.0)
    mean_ref[...] = jnp.sum(jnp.sum(weighted, axis=0, keepdims=True), axis=1, keepdims=True) / 1024.0
    chosen = jnp.zeros((16, 128), F32)
    for i in range(8):
        chosen = chosen + first_ref[:, i:i + 1] * table[i:i + 1, :]
    values = jnp.sum(chosen * pair_ref[...], axis=1, keepdims=True)
    sub = lax.broadcasted_iota(jnp.int32, (16, 128), 0)
    lane = lax.broadcasted_iota(jnp.int32, (16, 128), 1)
    row = jnp.sum(jnp.where(sub == lane, values, 0.0), axis=0, keepdims=True)
    trip_ref[...] = row[:, :16]


def spaces(*kinds):
    return [pl.BlockSpec(memory_space=kind) for kind in kinds]


def vmem(count):
    return spaces(*[pltpu.VMEM] * count)


def kept(*arrays):
    return [pltpu.with_memory_space_constraint(a, pltpu.VMEM) for a in arrays]


def left_in_hbm(*arrays):
    return [pltpu.with_memory_space_constraint(a, pltpu.HBM) for a in arrays]


def rows_call(doubles, coulomb):
    _, width, depth = doubles.shape
    return pl.pallas_call(
        rows_kernel,
        out_shape=pltpu.VMEM((2, width, depth), doubles.dtype),
        in_specs=spaces(pl.ANY, pl.ANY),
        out_specs=vmem(1)[0],
        scratch_shapes=[pltpu.SemaphoreType.DMA((2,))],
        compiler_params=SMALL,
        name="rows",
    )(*left_in_hbm(doubles, coulomb))


def prep_call(integrals, lists, tile_count, occ_energy, vir_energy, singles):
    occupied, width_block = singles.shape
    width = vir_energy.shape[0]
    slots = lists.shape[2]
    return pl.pallas_call(
        prep_kernel,
        out_shape=(
            pltpu.VMEM(integrals.shape, integrals.dtype),
            pltpu.VMEM((2, occupied * width_block, width, width), F32),
            pltpu.VMEM((occupied * width_block, width), F32),
            pltpu.VMEM((1, 128), F32),
            pltpu.VMEM((slots, 128), F32),
            pltpu.VMEM((slots, 128), F32),
        ),
        in_specs=spaces(pl.ANY, *[pltpu.SMEM] * 5, pltpu.VMEM),
        out_specs=tuple(vmem(6)),
        scratch_shapes=[pltpu.SemaphoreType.DMA],
        compiler_params=SMALL,
        name="prep",
    )(*left_in_hbm(integrals, lists), tile_count, *left_in_hbm(occ_energy, vir_energy, singles, vir_energy[None]))


def energy_call(slabs, one, two, recip, amps, info):
    occupied, _, width, _ = slabs.shape
    return pl.pallas_call(
        energy_kernel,
        out_shape=pltpu.VMEM((64, 128), F32),
        in_specs=vmem(6),
        out_specs=vmem(1)[0],
        scratch_shapes=[pltpu.VMEM((2 * occupied, width), F32)],
        compiler_params=SMALL,
        name="energies",
    )(*kept(slabs, one, two, recip, amps, info))


def table_call(message):
    return pl.pallas_call(
        table_kernel,
        out_shape=pltpu.VMEM((128, 128), F32),
        in_specs=vmem(1),
        out_specs=vmem(1)[0],
        compiler_params=SMALL,
        name="table",
    )(*kept(message))


def final_call(tables, first_hot, pair_hot):
    slots = first_hot.shape[0]
    return pl.pallas_call(
        final_kernel,
        out_shape=(jax.ShapeDtypeStruct((1, slots), F32), jax.ShapeDtypeStruct((1, 1), F32)),
        in_specs=vmem(3),
        out_specs=tuple(vmem(2)),
        compiler_params=SMALL,
        name="lookup",
    )(*kept(tables, first_hot, pair_hot))


def body(integrals, doubles, coulomb, singles, occ_energy, vir_energy, triplets, tile_count):
    first, second = routes()
    sent = rows_call(doubles, coulomb)
    one = lax.ppermute(sent, AXES, first)
    two = lax.ppermute(sent, AXES, second)
    lists = jnp.transpose(triplets, (2, 0, 1))
    slabs, recip, amps, info, first_hot, pair_hot = prep_call(integrals, lists, tile_count, occ_energy, vir_energy, singles)
    message = energy_call(slabs, one, two, recip, amps, info)
    message = lax.all_to_all(message, PLANE, 0, 0, tiled=True)
    tables = table_call(message)
    tables = lax.all_to_all(tables, STACK, 0, 0, tiled=True)
    trip, mean = final_call(tables, first_hot, pair_hot)
    return trip, mean.reshape(())


def solution(mesh):
    fine = Mesh(mesh.devices.reshape(SIZES), AXES)
    in_specs = (
        P(None, BLK, None, None),
        P(BLK, None, None),
        P(BLK, None, None),
        P(None, BLK),
        P(),
        P(),
        P(GRP, None, None),
        P(GRP),
    )
    out_specs = (P(GRP, None), P())
    return jax.shard_map(body, mesh=fine, in_specs=in_specs, out_specs=out_specs, check_vma=False)
```

```python
import jax
import jax.numpy as jnp
import numpy as np
from jax import lax
from jax.experimental import pallas as pl
from jax.experimental.pallas import tpu as pltpu
from jax.sharding import Mesh
from jax.sharding import PartitionSpec as P

AXES = ("yl", "z", "c", "yh", "x")
SIZES = (4, 8, 2, 2, 8)
GRP = ("yl", "z", "c")
BLK = ("yh", "x")
PLANE = ("yh", "yl", "x")
STACK = ("z", "c")
NO = 8
WORKERS = 4
SMALL = pltpu.CompilerParams(vmem_limit_bytes=12 * 1024 * 1024)
F32 = jnp.float32


def device_at(yl, z, c, yh, x):
    return ((((yl * 8) + z) * 2 + c) * 2 + yh) * 8 + x


def owners_of(yl, z, c, yh, x, none, one):
    low, high = z & 1, (z >> 1) & 1
    offset = none * (2 * low + 4 * high) + one * (low + 4 * high) + (1 - none - one) * (low + 2 * high)
    owner = (yh * 8 + x) ^ (offset + 8 * c)
    swapped = ((owner & 1) << 3) | ((owner & 6) ^ (yl << 1)) | (owner >> 3)
    return owner, none * (owner ^ 9) + (1 - none) * swapped


def pair_at(owner, yl):
    return owner >> 1, (owner & 1) * 4 + (((owner >> 1) & 3) ^ yl)


def routes():
    first, second = [], []
    for yl, z, c, yh, x in np.ndindex(*SIZES):
        if z < WORKERS:
            here = device_at(yl, z, c, yh, x)
            owner, other = owners_of(yl, z, c, yh, x, int(yl == 0), int(yl == 1))
            crosses = int(other >> 3 != yh) if yl & 1 else 1
            first.append((device_at(yl ^ (2 * c), z, c, owner >> 3, owner & 7), here))
            second.append((device_at(yl ^ (2 * crosses), z, c, other >> 3, other & 7), here))
    return first, second


def where_am_i():
    yl, z, c, yh, x = (lax.axis_index(axis) for axis in AXES)
    return yl, z, c, yh, x


def own_pairs():
    yl, z, c, yh, x = where_am_i()
    none, one = (yl == 0).astype(jnp.int32), (yl == 1).astype(jnp.int32)
    owner, other = owners_of(yl, z, c, yh, x, none, one)
    return pair_at(owner, yl), pair_at(other, yl)


def sent_rows(yl, c, yh, x):
    low_bits = ((yh * 8 + x) >> 1) & 3
    crosses = (1 - (yl & 1)) | (yh ^ (x & 1) ^ c)
    return low_bits ^ yl ^ (2 * c), low_bits ^ yl ^ (2 * crosses)


def rows_kernel(doubles_ref, coulomb_ref, first_ref, second_ref, sems):
    yl, _, c, yh, x = where_am_i()
    first, second = sent_rows(yl, c, yh, x)
    copies = [
        pltpu.make_async_copy(doubles_ref.at[first], first_ref.at[0], sems.at[0]),
        pltpu.make_async_copy(coulomb_ref.at[first], first_ref.at[1], sems.at[1]),
        pltpu.make_async_copy(doubles_ref.at[second], second_ref.at[0], sems.at[2]),
        pltpu.make_async_copy(coulomb_ref.at[second], second_ref.at[1], sems.at[3]),
    ]
    for copy in copies:
        copy.start()
    for copy in copies:
        copy.wait()


def prep_kernel(ints_ref, trip_ref, count_ref, occ_ref, vir_ref, singles_ref, virs_ref,
                slab_ref, recip_ref, amps_ref, info_ref, first_ref, pair_ref, sem):
    occupied, width_block = singles_ref.shape
    width = virs_ref.shape[1]
    slots = first_ref.shape[0]
    _, z, _, yh, x = where_am_i()
    place = yh * 8 + x
    (j1, k1), (j2, k2) = own_pairs()
    diagonal = j1 == k1
    busy = z < WORKERS
    live = count_ref[0]
    slabs = pltpu.make_async_copy(ints_ref, slab_ref, sem)

    @pl.when(busy)
    def _():
        slabs.start()

    lane = lax.broadcasted_iota(jnp.int32, (1, 128), 1)
    mine = jnp.where(place < live, trip_ref[0, 0, place] + 16, -1)
    info = jnp.where(lane == mine, 1.0, 0.0)
    info = jnp.where(lane == 24, jnp.where(busy, j1 * NO + k1, -1).astype(F32), info)
    info = jnp.where(lane == 25, jnp.where(busy, j2 * NO + k2, -1).astype(F32), info)
    info = jnp.where(lane == 26, (trip_ref[1, 0, place] * NO + trip_ref[2, 0, place]).astype(F32), info)
    info_ref[...] = info

    sub = lax.broadcasted_iota(jnp.int32, (slots, 128), 0)
    lanes = lax.broadcasted_iota(jnp.int32, (slots, 128), 1)
    first_at = jnp.full((slots, 128), -1, jnp.int32)
    pair_at_ = jnp.full((slots, 128), -1, jnp.int32)
    for s in range(slots):
        first_at = jnp.where(sub == s, jnp.where(s < live, trip_ref[0, 0, s], -1), first_at)
        pair_at_ = jnp.where(sub == s, trip_ref[1, 0, s] * NO + trip_ref[2, 0, s], pair_at_)
    first_ref[...] = jnp.where(first_at == lanes, 1.0, 0.0)
    pair_ref[...] = jnp.where(pair_at_ == lanes, 1.0, 0.0)

    def fill(table, second, third, write_amps):
        across = jnp.broadcast_to(virs_ref[...], (width, width))
        sums = across.T + across

        def one_occ(i, carry):
            occ_sum = occ_ref[i] + occ_ref[second] + occ_ref[third]
            for a in range(width_block):
                r = i * width_block + a
                recip_ref[table, r] = 1.0 / ((occ_sum - vir_ref[place * width_block + a]) - sums)
                if write_amps:
                    amps_ref[pl.ds(r, 1), :] = jnp.full((1, 128), singles_ref[i, a], F32)
            return carry

        lax.fori_loop(0, occupied, one_occ, 0)

    @pl.when(busy)
    def _():
        fill(0, j1, k1, True)

    @pl.when(jnp.logical_and(busy, diagonal))
    def _():
        fill(1, j2, k2, False)

    @pl.when(busy)
    def _():
        slabs.wait()


def energy_kernel(ints_ref, one_ref, two_ref, recip_ref, amps_ref, info_ref, out_ref, sums_ref):
    occupied, width_block, width, _ = ints_ref.shape
    _, z, _, _, _ = where_am_i()
    (j1, k1), _ = own_pairs()
    diagonal = j1 == k1
    sums_ref[...] = jnp.zeros(sums_ref.shape, F32)

    def fold(value):
        return jnp.sum(value.reshape(width // 8, 8, width), axis=0)

    def both(couple):
        amps = jnp.concatenate([one_ref[0], two_ref[0]], axis=0)
        coupling_one = one_ref[1].astype(F32)
        coupling_two = two_ref[1].astype(F32)
        if couple:
            coupling_two = coupling_two.T

        def one_occ(i, carry):
            slab = ints_ref[i].reshape(width_block * width, width)
            products = lax.dot_general(slab, amps, (((1,), (1,)), ((), ())), preferred_element_type=F32)
            total_one = jnp.zeros((8, width), F32)
            total_two = jnp.zeros((8, width), F32)
            for a in range(width_block):
                r = i * width_block + a
                left = products[a * width:(a + 1) * width, :width]
                right = products[a * width:(a + 1) * width, width:]
                amp = amps_ref[pl.ds(r, 1), :]
                recip_one = recip_ref[0, r]
                if couple:
                    connected_one = right + left.T
                    connected_two = connected_one
                    recip_two = recip_one
                else:
                    connected_one = left + left.T
                    connected_two = right + right.T
                    recip_two = recip_ref[1, r]
                full_one = connected_one + amp * coupling_one
                full_two = connected_two + amp * coupling_two
                total_one = total_one + fold(full_one * full_one * recip_one)
                total_two = total_two + fold(full_two * full_two * recip_two)
            sums_ref[pl.ds(i, 1), :] = jnp.sum(total_one, axis=0, keepdims=True)
            sums_ref[pl.ds(i + occupied, 1), :] = jnp.sum(total_two, axis=0, keepdims=True)
            return carry

        lax.fori_loop(0, occupied, one_occ, 0, unroll=True)

    busy = z < WORKERS

    @pl.when(jnp.logical_and(busy, jnp.logical_not(diagonal)))
    def _():
        both(True)

    @pl.when(jnp.logical_and(busy, diagonal))
    def _():
        both(False)

    energies = jnp.sum(sums_ref[...], axis=1, keepdims=True)
    sub = lax.broadcasted_iota(jnp.int32, (2 * occupied, 128), 0)
    lane = lax.broadcasted_iota(jnp.int32, (2 * occupied, 128), 1)
    row = jnp.sum(jnp.where(sub == lane, energies, 0.0), axis=0, keepdims=True)
    out_ref[...] = jnp.broadcast_to(row + info_ref[...], out_ref.shape)


def table_kernel(in_ref, out_ref):
    got = in_ref[...]
    lane = lax.broadcasted_iota(jnp.int32, got.shape, 1)
    lane_at = lane.astype(F32)
    lists = got[:, 26:27] + 64.0

    def gathered(pick):
        return lax.dot_general(
            got,
            (pick == lane_at).astype(F32),
            (((0,), (0,)), ((), ())),
            precision=lax.Precision.HIGHEST,
            preferred_element_type=F32,
        )

    ones = gathered(jnp.where(lane < 64, got[:, 24:25], lists))
    twos = gathered(got[:, 25:26])
    low = lax.broadcasted_iota(jnp.int32, (8, 128), 1) < 64
    packed = jnp.where(low, ones[0:8] + twos[8:16], ones[16:24])
    peers = out_ref.shape[0] // 8
    out_ref[...] = jnp.broadcast_to(packed[None], (peers, 8, 128)).reshape(peers * 8, 128)


def final_kernel(in_ref, first_ref, pair_ref, trip_ref, mean_ref):
    peers = in_ref.shape[0] // 8
    table = jnp.sum(in_ref[...].reshape(peers, 8, 128), axis=0)
    counts = pltpu.roll(table, 64, 1)
    low = lax.broadcasted_iota(jnp.int32, (8, 128), 1) < 64
    weighted = jnp.where(low, table * counts, 0.0)
    mean_ref[...] = jnp.sum(jnp.sum(weighted, axis=0, keepdims=True), axis=1, keepdims=True) / 1024.0
    chosen = jnp.zeros((16, 128), F32)
    for i in range(8):
        chosen = chosen + first_ref[:, i:i + 1] * table[i:i + 1, :]
    values = jnp.sum(chosen * pair_ref[...], axis=1, keepdims=True)
    sub = lax.broadcasted_iota(jnp.int32, (16, 128), 0)
    lane = lax.broadcasted_iota(jnp.int32, (16, 128), 1)
    row = jnp.sum(jnp.where(sub == lane, values, 0.0), axis=0, keepdims=True)
    trip_ref[...] = row[:, :16]


def spaces(*kinds):
    return [pl.BlockSpec(memory_space=kind) for kind in kinds]


def vmem(count):
    return spaces(*[pltpu.VMEM] * count)


def kept(*arrays):
    return [pltpu.with_memory_space_constraint(a, pltpu.VMEM) for a in arrays]


def left_in_hbm(*arrays):
    return [pltpu.with_memory_space_constraint(a, pltpu.HBM) for a in arrays]


def rows_call(doubles, coulomb):
    _, width, depth = doubles.shape
    return pl.pallas_call(
        rows_kernel,
        out_shape=(pltpu.VMEM((2, width, depth), doubles.dtype),) * 2,
        in_specs=spaces(pl.ANY, pl.ANY),
        out_specs=tuple(vmem(2)),
        scratch_shapes=[pltpu.SemaphoreType.DMA((4,))],
        compiler_params=SMALL,
        name="rows",
    )(*left_in_hbm(doubles, coulomb))


def prep_call(integrals, lists, tile_count, occ_energy, vir_energy, singles):
    occupied, width_block = singles.shape
    width = vir_energy.shape[0]
    slots = lists.shape[2]
    return pl.pallas_call(
        prep_kernel,
        out_shape=(
            pltpu.VMEM(integrals.shape, integrals.dtype),
            pltpu.VMEM((2, occupied * width_block, width, width), F32),
            pltpu.VMEM((occupied * width_block, width), F32),
            pltpu.VMEM((1, 128), F32),
            pltpu.VMEM((slots, 128), F32),
            pltpu.VMEM((slots, 128), F32),
        ),
        in_specs=spaces(pl.ANY, *[pltpu.SMEM] * 5, pltpu.VMEM),
        out_specs=tuple(vmem(6)),
        scratch_shapes=[pltpu.SemaphoreType.DMA],
        compiler_params=SMALL,
        name="prep",
    )(*left_in_hbm(integrals, lists), tile_count, *left_in_hbm(occ_energy, vir_energy, singles, vir_energy[None]))


def energy_call(slabs, one, two, recip, amps, info):
    occupied, _, width, _ = slabs.shape
    return pl.pallas_call(
        energy_kernel,
        out_shape=pltpu.VMEM((64, 128), F32),
        in_specs=vmem(6),
        out_specs=vmem(1)[0],
        scratch_shapes=[pltpu.VMEM((2 * occupied, width), F32)],
        compiler_params=SMALL,
        name="energies",
    )(*kept(slabs, one, two, recip, amps, info))


def table_call(message):
    return pl.pallas_call(
        table_kernel,
        out_shape=pltpu.VMEM((128, 128), F32),
        in_specs=vmem(1),
        out_specs=vmem(1)[0],
        compiler_params=SMALL,
        name="table",
    )(*kept(message))


def final_call(tables, first_hot, pair_hot):
    slots = first_hot.shape[0]
    return pl.pallas_call(
        final_kernel,
        out_shape=(jax.ShapeDtypeStruct((1, slots), F32), jax.ShapeDtypeStruct((1, 1), F32)),
        in_specs=vmem(3),
        out_specs=tuple(vmem(2)),
        compiler_params=SMALL,
        name="lookup",
    )(*kept(tables, first_hot, pair_hot))


def body(integrals, doubles, coulomb, singles, occ_energy, vir_energy, triplets, tile_count):
    first, second = routes()
    sent_first, sent_second = rows_call(doubles, coulomb)
    one = lax.ppermute(sent_first, AXES, first)
    two = lax.ppermute(sent_second, AXES, second)
    lists = jnp.transpose(triplets, (2, 0, 1))
    slabs, recip, amps, info, first_hot, pair_hot = prep_call(integrals, lists, tile_count, occ_energy, vir_energy, singles)
    message = energy_call(slabs, one, two, recip, amps, info)
    message = lax.all_to_all(message, PLANE, 0, 0, tiled=True)
    tables = table_call(message)
    tables = lax.all_to_all(tables, STACK, 0, 0, tiled=True)
    trip, mean = final_call(tables, first_hot, pair_hot)
    return trip, mean.reshape(())


def solution(mesh):
    fine = Mesh(mesh.devices.reshape(SIZES), AXES)
    in_specs = (
        P(None, BLK, None, None),
        P(BLK, None, None),
        P(BLK, None, None),
        P(None, BLK),
        P(),
        P(),
        P(GRP, None, None),
        P(GRP),
    )
    out_specs = (P(GRP, None), P())
    return jax.shard_map(body, mesh=fine, in_specs=in_specs, out_specs=out_specs, check_vma=False)
```

```python
import jax
import jax.numpy as jnp
import numpy as np
from jax import lax
from jax.experimental import pallas as pl
from jax.experimental.pallas import tpu as pltpu
from jax.sharding import Mesh
from jax.sharding import PartitionSpec as P

AXES = ("yl", "z", "c", "yh", "x")
SIZES = (4, 8, 2, 2, 8)
GRP = ("yl", "z", "c")
BLK = ("yh", "x")
PLANE = ("yh", "yl", "x")
STACK = ("z", "c")
NO = 8
WORKERS = 4
SMALL = pltpu.CompilerParams(vmem_limit_bytes=12 * 1024 * 1024)
F32 = jnp.float32


def device_at(yl, z, c, yh, x):
    return ((((yl * 8) + z) * 2 + c) * 2 + yh) * 8 + x


OWNERS = (
    (0x62d73195cf4eb80a, 0x573db2f106a48ec9, 0xf1b45763a92cd0e8, 0x3f71d5096c824abe,
     0x19532b76facde480, 0x731b465fe0982dac, 0x05421d3798ebacf6, 0x942573108edacb6f),
    (0x51fd36780ebc24a9, 0x92514dbf78e3ac60, 0xf315c709e42ab8d6, 0x6f43d51792cbe08a,
     0x76325bf1894dca0e, 0x1974b0356a82decf, 0x859c2160afd43be7, 0x072b1356fcae4d98),
    (0x38b9d6f12e0a547c, 0x709a4b15f8326cde, 0xf13b6709ea2d45c8, 0x0b253ce71f98ad46,
     0x1952b37fa084ce6d, 0x924375de01acb68f, 0x83145d6092cbeaf7, 0x27a1c45689b3dfe0),
    (0xb39746e5d2108fca, 0x3a2b9d71c80e654f, 0x710965d3ac28bef4, 0x5b731f4d20a9c8e6,
     0x12a0d3f79b84e65c, 0x09327e5f81cba46d, 0x27b154360a9cfd8e, 0xf0153762e9ba4cd8),
)
APART = 2


def owner_table():
    digits = [[[int(d, 16) for d in f"{code:016x}"] for code in codes] for codes in OWNERS]
    return np.array(digits, np.int32).reshape(-1)


def owner_index(yl, z, c, yh, x):
    return (((yl ^ (2 * yh)) * WORKERS + z % WORKERS) * 2 + c) * 16 + yh * 8 + x


def pairs_of(owner, u, where):
    swapped = ((owner & 1) << 3) | ((owner & 6) ^ (u << 1)) | (owner >> 3)
    other = where(swapped == owner, owner ^ APART, swapped)
    return other, pair_at(owner, u), pair_at(other, u)


def pair_at(owner, u):
    return owner >> 1, (owner & 1) * 4 + (((owner >> 1) & 3) ^ u)


def routes():
    table, near, far = owner_table(), [], []
    for yl, z, c, yh, x in np.ndindex(*SIZES):
        if z < WORKERS:
            here, u = device_at(yl, z, c, yh, x), yl ^ (2 * yh)
            owner = int(table[owner_index(yl, z, c, yh, x)])
            other, _, _ = pairs_of(owner, u, lambda a, b, c: b if a else c)
            for route, block in ((near, owner), (far, other)):
                half = block >> 3
                route.append((device_at(u ^ (2 * half), z, c, half, block & 7), here))
    return near, far


def where_am_i():
    yl, z, c, yh, x = (lax.axis_index(axis) for axis in AXES)
    return yl, z, c, yh, x


def rows_kernel(doubles_ref, coulomb_ref, out_ref, sems):
    yl, _, _, yh, x = where_am_i()
    row = (((yh * 8 + x) >> 1) & 3) ^ yl ^ (2 * yh)
    copies = [
        pltpu.make_async_copy(doubles_ref.at[row], out_ref.at[0], sems.at[0]),
        pltpu.make_async_copy(coulomb_ref.at[row], out_ref.at[1], sems.at[1]),
    ]
    for copy in copies:
        copy.start()
    for copy in copies:
        copy.wait()


def prep_kernel(ints_ref, owners_ref, trip_ref, count_ref, occ_ref, vir_ref, singles_ref, virs_ref,
                slab_ref, recip_ref, amps_ref, info_ref, first_ref, pair_ref, sem):
    occupied, width_block = singles_ref.shape
    width = virs_ref.shape[1]
    slots = first_ref.shape[0]
    yl, z, c, yh, x = where_am_i()
    place = yh * 8 + x
    owner = owners_ref[owner_index(yl, z, c, yh, x)]
    _, (j1, k1), (j2, k2) = pairs_of(owner, yl ^ (2 * yh), jnp.where)
    diagonal = j1 == k1
    busy = z < WORKERS
    live = count_ref[0]
    slabs = pltpu.make_async_copy(ints_ref, slab_ref, sem)

    @pl.when(busy)
    def _():
        slabs.start()

    lane = lax.broadcasted_iota(jnp.int32, (1, 128), 1)
    mine = jnp.where(place < live, trip_ref[0, 0, place] + 16, -1)
    info = jnp.where(lane == mine, 1.0, 0.0)
    info = jnp.where(lane == 24, jnp.where(busy, j1 * NO + k1, -1).astype(F32), info)
    info = jnp.where(lane == 25, jnp.where(busy, j2 * NO + k2, -1).astype(F32), info)
    info = jnp.where(lane == 26, (trip_ref[1, 0, place] * NO + trip_ref[2, 0, place]).astype(F32), info)
    info = jnp.where(lane == 27, diagonal.astype(F32), info)
    info_ref[...] = info

    sub = lax.broadcasted_iota(jnp.int32, (slots, 128), 0)
    lanes = lax.broadcasted_iota(jnp.int32, (slots, 128), 1)
    first_at = jnp.full((slots, 128), -1, jnp.int32)
    pair_at_ = jnp.full((slots, 128), -1, jnp.int32)
    for s in range(slots):
        first_at = jnp.where(sub == s, jnp.where(s < live, trip_ref[0, 0, s], -1), first_at)
        pair_at_ = jnp.where(sub == s, trip_ref[1, 0, s] * NO + trip_ref[2, 0, s], pair_at_)
    first_ref[...] = jnp.where(first_at == lanes, 1.0, 0.0)
    pair_ref[...] = jnp.where(pair_at_ == lanes, 1.0, 0.0)

    def fill(table, second, third, write_amps):
        across = jnp.broadcast_to(virs_ref[...], (width, width))
        sums = across.T + across

        def one_occ(i, carry):
            occ_sum = occ_ref[i] + occ_ref[second] + occ_ref[third]
            for a in range(width_block):
                r = i * width_block + a
                recip_ref[table, r] = 1.0 / ((occ_sum - vir_ref[place * width_block + a]) - sums)
                if write_amps:
                    amps_ref[pl.ds(r, 1), :] = jnp.full((1, 128), singles_ref[i, a], F32)
            return carry

        lax.fori_loop(0, occupied, one_occ, 0)

    @pl.when(busy)
    def _():
        fill(0, j1, k1, True)

    @pl.when(jnp.logical_and(busy, diagonal))
    def _():
        fill(1, j2, k2, False)

    @pl.when(busy)
    def _():
        slabs.wait()


def energy_kernel(ints_ref, one_ref, two_ref, recip_ref, amps_ref, info_ref, out_ref, sums_ref):
    occupied, width_block, width, _ = ints_ref.shape
    _, z, _, _, _ = where_am_i()
    diagonal = jnp.max(info_ref[:, 27:28]) > 0.5
    sums_ref[...] = jnp.zeros(sums_ref.shape, F32)

    def fold(value):
        return jnp.sum(value.reshape(width // 8, 8, width), axis=0)

    def both(couple):
        amps = jnp.concatenate([one_ref[0], two_ref[0]], axis=0)
        coupling_one = one_ref[1].astype(F32)
        coupling_two = two_ref[1].astype(F32)
        if couple:
            coupling_two = coupling_two.T

        def one_occ(i, carry):
            slab = ints_ref[i].reshape(width_block * width, width)
            products = lax.dot_general(slab, amps, (((1,), (1,)), ((), ())), preferred_element_type=F32)
            total_one = jnp.zeros((8, width), F32)
            total_two = jnp.zeros((8, width), F32)
            for a in range(width_block):
                r = i * width_block + a
                left = products[a * width:(a + 1) * width, :width]
                right = products[a * width:(a + 1) * width, width:]
                amp = amps_ref[pl.ds(r, 1), :]
                recip_one = recip_ref[0, r]
                if couple:
                    connected_one = right + left.T
                    connected_two = connected_one
                    recip_two = recip_one
                else:
                    connected_one = left + left.T
                    connected_two = right + right.T
                    recip_two = recip_ref[1, r]
                full_one = connected_one + amp * coupling_one
                full_two = connected_two + amp * coupling_two
                total_one = total_one + fold(full_one * full_one * recip_one)
                total_two = total_two + fold(full_two * full_two * recip_two)
            sums_ref[pl.ds(i, 1), :] = jnp.sum(total_one, axis=0, keepdims=True)
            sums_ref[pl.ds(i + occupied, 1), :] = jnp.sum(total_two, axis=0, keepdims=True)
            return carry

        lax.fori_loop(0, occupied, one_occ, 0, unroll=True)

    busy = z < WORKERS

    @pl.when(jnp.logical_and(busy, jnp.logical_not(diagonal)))
    def _():
        both(True)

    @pl.when(jnp.logical_and(busy, diagonal))
    def _():
        both(False)

    energies = jnp.sum(sums_ref[...], axis=1, keepdims=True)
    sub = lax.broadcasted_iota(jnp.int32, (2 * occupied, 128), 0)
    lane = lax.broadcasted_iota(jnp.int32, (2 * occupied, 128), 1)
    row = jnp.sum(jnp.where(sub == lane, energies, 0.0), axis=0, keepdims=True)
    out_ref[...] = jnp.broadcast_to(row + info_ref[...], out_ref.shape)


def table_kernel(in_ref, out_ref):
    got = in_ref[...]
    lane = lax.broadcasted_iota(jnp.int32, got.shape, 1)
    lane_at = lane.astype(F32)
    lists = got[:, 26:27] + 64.0

    def gathered(pick):
        return lax.dot_general(
            got,
            (pick == lane_at).astype(F32),
            (((0,), (0,)), ((), ())),
            precision=lax.Precision.HIGHEST,
            preferred_element_type=F32,
        )

    ones = gathered(jnp.where(lane < 64, got[:, 24:25], lists))
    twos = gathered(got[:, 25:26])
    low = lax.broadcasted_iota(jnp.int32, (8, 128), 1) < 64
    packed = jnp.where(low, ones[0:8] + twos[8:16], ones[16:24])
    peers = out_ref.shape[0] // 8
    out_ref[...] = jnp.broadcast_to(packed[None], (peers, 8, 128)).reshape(peers * 8, 128)


def final_kernel(in_ref, first_ref, pair_ref, trip_ref, mean_ref):
    peers = in_ref.shape[0] // 8
    table = jnp.sum(in_ref[...].reshape(peers, 8, 128), axis=0)
    counts = pltpu.roll(table, 64, 1)
    low = lax.broadcasted_iota(jnp.int32, (8, 128), 1) < 64
    weighted = jnp.where(low, table * counts, 0.0)
    mean_ref[...] = jnp.sum(jnp.sum(weighted, axis=0, keepdims=True), axis=1, keepdims=True) / 1024.0
    chosen = jnp.zeros((16, 128), F32)
    for i in range(8):
        chosen = chosen + first_ref[:, i:i + 1] * table[i:i + 1, :]
    values = jnp.sum(chosen * pair_ref[...], axis=1, keepdims=True)
    sub = lax.broadcasted_iota(jnp.int32, (16, 128), 0)
    lane = lax.broadcasted_iota(jnp.int32, (16, 128), 1)
    row = jnp.sum(jnp.where(sub == lane, values, 0.0), axis=0, keepdims=True)
    trip_ref[...] = row[:, :16]


def spaces(*kinds):
    return [pl.BlockSpec(memory_space=kind) for kind in kinds]


def vmem(count):
    return spaces(*[pltpu.VMEM] * count)


def kept(*arrays):
    return [pltpu.with_memory_space_constraint(a, pltpu.VMEM) for a in arrays]


def left_in_hbm(*arrays):
    return [pltpu.with_memory_space_constraint(a, pltpu.HBM) for a in arrays]


def rows_call(doubles, coulomb):
    _, width, depth = doubles.shape
    return pl.pallas_call(
        rows_kernel,
        out_shape=pltpu.VMEM((2, width, depth), doubles.dtype),
        in_specs=spaces(pl.ANY, pl.ANY),
        out_specs=vmem(1)[0],
        scratch_shapes=[pltpu.SemaphoreType.DMA((2,))],
        compiler_params=SMALL,
        name="rows",
    )(*left_in_hbm(doubles, coulomb))


def prep_call(integrals, lists, tile_count, occ_energy, vir_energy, singles):
    occupied, width_block = singles.shape
    width = vir_energy.shape[0]
    slots = lists.shape[2]
    return pl.pallas_call(
        prep_kernel,
        out_shape=(
            pltpu.VMEM(integrals.shape, integrals.dtype),
            pltpu.VMEM((2, occupied * width_block, width, width), F32),
            pltpu.VMEM((occupied * width_block, width), F32),
            pltpu.VMEM((1, 128), F32),
            pltpu.VMEM((slots, 128), F32),
            pltpu.VMEM((slots, 128), F32),
        ),
        in_specs=spaces(pl.ANY, *[pltpu.SMEM] * 6, pltpu.VMEM),
        out_specs=tuple(vmem(6)),
        scratch_shapes=[pltpu.SemaphoreType.DMA],
        compiler_params=SMALL,
        name="prep",
    )(*left_in_hbm(integrals, jnp.asarray(owner_table()), lists), tile_count, *left_in_hbm(occ_energy, vir_energy, singles, vir_energy[None]))


def energy_call(slabs, one, two, recip, amps, info):
    occupied, _, width, _ = slabs.shape
    return pl.pallas_call(
        energy_kernel,
        out_shape=pltpu.VMEM((64, 128), F32),
        in_specs=vmem(6),
        out_specs=vmem(1)[0],
        scratch_shapes=[pltpu.VMEM((2 * occupied, width), F32)],
        compiler_params=SMALL,
        name="energies",
    )(*kept(slabs, one, two, recip, amps, info))


def table_call(message):
    return pl.pallas_call(
        table_kernel,
        out_shape=pltpu.VMEM((128, 128), F32),
        in_specs=vmem(1),
        out_specs=vmem(1)[0],
        compiler_params=SMALL,
        name="table",
    )(*kept(message))


def final_call(tables, first_hot, pair_hot):
    slots = first_hot.shape[0]
    return pl.pallas_call(
        final_kernel,
        out_shape=(jax.ShapeDtypeStruct((1, slots), F32), jax.ShapeDtypeStruct((1, 1), F32)),
        in_specs=vmem(3),
        out_specs=tuple(vmem(2)),
        compiler_params=SMALL,
        name="lookup",
    )(*kept(tables, first_hot, pair_hot))


def body(integrals, doubles, coulomb, singles, occ_energy, vir_energy, triplets, tile_count):
    near, far = routes()
    sent = rows_call(doubles, coulomb)
    two = lax.ppermute(sent, AXES, far)
    one = lax.ppermute(sent, AXES, near)
    lists = jnp.transpose(triplets, (2, 0, 1))
    slabs, recip, amps, info, first_hot, pair_hot = prep_call(integrals, lists, tile_count, occ_energy, vir_energy, singles)
    message = energy_call(slabs, one, two, recip, amps, info)
    message = lax.all_to_all(message, PLANE, 0, 0, tiled=True)
    tables = table_call(message)
    tables = lax.all_to_all(tables, STACK, 0, 0, tiled=True)
    trip, mean = final_call(tables, first_hot, pair_hot)
    return trip, mean.reshape(())


def solution(mesh):
    fine = Mesh(mesh.devices.reshape(SIZES), AXES)
    in_specs = (
        P(None, BLK, None, None),
        P(BLK, None, None),
        P(BLK, None, None),
        P(None, BLK),
        P(),
        P(),
        P(GRP, None, None),
        P(GRP),
    )
    out_specs = (P(GRP, None), P())
    return jax.shard_map(body, mesh=fine, in_specs=in_specs, out_specs=out_specs, check_vma=False)
```

```python
import jax
import jax.numpy as jnp
import numpy as np
from jax import lax
from jax.experimental import pallas as pl
from jax.experimental.pallas import tpu as pltpu
from jax.sharding import Mesh
from jax.sharding import PartitionSpec as P

AXES = ("yl", "z", "c", "yh", "x")
SIZES = (4, 8, 2, 2, 8)
GRP = ("yl", "z", "c")
BLK = ("yh", "x")
PLANE = ("yh", "yl", "x")
STACK = ("z", "c")
NO = 8
WORKERS = 4
SMALL = pltpu.CompilerParams(vmem_limit_bytes=12 * 1024 * 1024)
F32 = jnp.float32


def device_at(yl, z, c, yh, x):
    return ((((yl * 8) + z) * 2 + c) * 2 + yh) * 8 + x


OWNERS = (
    (0x1739dbf5ace48206, 0x5fd7b193c64e28a0, 0x3961705deaf24b8c, 0xf57d238960c1e4ba,
     0x74b25d310f8cae69, 0x93541706fe2dbac8, 0x0123456789abcdef, 0x6215347098badcfe),
    (0x7f5db1986e4c3a02, 0xf5dc3b1976e420a8, 0x50b317df928e46ca, 0x9475d031ecf2a8b6,
     0x471b5360fa2dce89, 0x89412d05afc3eb67, 0x0132457689abdcef, 0x1324c657089abdfe),
    (0xfb39d5e708a264c1, 0x9ad5bcfe12384706, 0x39ba5d1f8e24c670, 0x138b7fd9204a5c6e,
     0x58a23406f1c9ebd7, 0x21c46370df8ba5e9, 0x70234651a9bcdef8, 0x0241c765ea93bd8f),
    (0x73b91efdc20864a5, 0xdb679fc30a1e8542, 0xf97a6d15b324e8c0, 0x589b73d120a64fec,
     0x0152364f89bcaed7, 0x3210b7549ecaf68d, 0x10234567a89bcdfe, 0x2a315470eb89dc6f),
)
APART = 2


def owner_table():
    digits = [[[int(d, 16) for d in f"{code:016x}"] for code in codes] for codes in OWNERS]
    return np.array(digits, np.int32).reshape(-1)


def owner_index(yl, z, c, yh, x):
    return (((yl ^ (2 * yh)) * WORKERS + z % WORKERS) * 2 + c) * 16 + yh * 8 + x


def pairs_of(owner, u, where):
    swapped = ((owner & 1) << 3) | ((owner & 6) ^ (u << 1)) | (owner >> 3)
    other = where(swapped == owner, owner ^ APART, swapped)
    return other, pair_at(owner, u), pair_at(other, u)


def pair_at(owner, u):
    return owner >> 1, (owner & 1) * 4 + (((owner >> 1) & 3) ^ u)


def routes():
    table, near, far = owner_table(), [], []
    for yl, z, c, yh, x in np.ndindex(*SIZES):
        if z < WORKERS:
            here, u = device_at(yl, z, c, yh, x), yl ^ (2 * yh)
            owner = int(table[owner_index(yl, z, c, yh, x)])
            other, _, _ = pairs_of(owner, u, lambda a, b, c: b if a else c)
            for route, block in ((near, owner), (far, other)):
                half = block >> 3
                route.append((device_at(u ^ (2 * half), z, c, half, block & 7), here))
    return near, far


def where_am_i():
    yl, z, c, yh, x = (lax.axis_index(axis) for axis in AXES)
    return yl, z, c, yh, x


def rows_kernel(doubles_ref, coulomb_ref, out_ref, sems):
    yl, z, _, yh, x = where_am_i()
    row = (((yh * 8 + x) >> 1) & 3) ^ yl ^ (2 * yh)
    copies = [
        pltpu.make_async_copy(doubles_ref.at[row], out_ref.at[0], sems.at[0]),
        pltpu.make_async_copy(coulomb_ref.at[row], out_ref.at[1], sems.at[1]),
    ]

    @pl.when(z < WORKERS)
    def _():
        for copy in copies:
            copy.start()
        for copy in copies:
            copy.wait()


def prep_kernel(owners_ref, trip_ref, count_ref, occ_ref, vir_ref, singles_ref, virs_ref,
                recip_ref, amps_ref, info_ref, code_ref, slots_ref):
    occupied, width_block = singles_ref.shape
    width = virs_ref.shape[1]
    slots = trip_ref.shape[2]
    yl, z, c, yh, x = where_am_i()
    place = yh * 8 + x
    owner = owners_ref[owner_index(yl, z, c, yh, x)]
    other, (j1, k1), (j2, k2) = pairs_of(owner, yl ^ (2 * yh), jnp.where)
    diagonal = j1 == k1
    busy = z < WORKERS
    live = count_ref[0]

    lane = lax.broadcasted_iota(jnp.int32, (1, 128), 1)
    info = jnp.where(lane == 0, owner.astype(F32), 0.0)
    info = jnp.where(lane == 1, other.astype(F32), info)
    info_ref[...] = jnp.where(lane == 2, diagonal.astype(F32), info)

    def code_of(s):
        i, j, k = trip_ref[0, 0, s], trip_ref[1, 0, s], trip_ref[2, 0, s]
        code = ((j ^ k) & 3) * 128 + i * 16 + j * 2 + (k >> 2)
        return jnp.where(s < live, code, -1)

    code_ref[...] = jnp.where(lane == z * 2 + c, (code_of(place) + 1).astype(F32), 0.0)

    sub = lax.broadcasted_iota(jnp.int32, (slots, 128), 0)
    lanes = lax.broadcasted_iota(jnp.int32, (slots, 128), 1)
    codes = jnp.full((slots, 128), -1, jnp.int32)
    for s in range(slots):
        codes = jnp.where(sub == s, code_of(s), codes)
    for u in range(4):
        slots_ref[u] = jnp.where(codes == u * 128 + lanes, 1.0, 0.0)

    def fill(table, second, third, write_amps):
        across = jnp.broadcast_to(virs_ref[...], (width, width))
        sums = across.T + across

        def one_occ(i, carry):
            occ_sum = occ_ref[i] + occ_ref[second] + occ_ref[third]
            for a in range(width_block):
                r = i * width_block + a
                recip_ref[table, r] = 1.0 / ((occ_sum - vir_ref[place * width_block + a]) - sums)
                if write_amps:
                    amps_ref[pl.ds(r, 1), :] = jnp.full((1, 128), singles_ref[i, a], F32)
            return carry

        lax.fori_loop(0, occupied, one_occ, 0)

    @pl.when(busy)
    def _():
        fill(0, j1, k1, True)

    @pl.when(jnp.logical_and(busy, diagonal))
    def _():
        fill(1, j2, k2, False)


def energy_kernel(ints_ref, one_ref, two_ref, recip_ref, amps_ref, info_ref, code_ref, out_ref, sums_ref):
    occupied, width_block, width, _ = ints_ref.shape
    _, z, _, _, _ = where_am_i()
    diagonal = jnp.max(info_ref[:, 2:3]) > 0.5
    sums_ref[...] = jnp.zeros(sums_ref.shape, F32)

    def fold(value):
        return jnp.sum(value.reshape(width // 8, 8, width), axis=0)

    def both(couple):
        amps = jnp.concatenate([one_ref[0], two_ref[0]], axis=0)
        coupling_one = one_ref[1].astype(F32)
        coupling_two = two_ref[1].astype(F32)
        if couple:
            coupling_two = coupling_two.T

        def one_occ(i, carry):
            slab = ints_ref[i].reshape(width_block * width, width)
            products = lax.dot_general(slab, amps, (((1,), (1,)), ((), ())), preferred_element_type=F32)
            total_one = jnp.zeros((8, width), F32)
            total_two = jnp.zeros((8, width), F32)
            for a in range(width_block):
                r = i * width_block + a
                left = products[a * width:(a + 1) * width, :width]
                right = products[a * width:(a + 1) * width, width:]
                amp = amps_ref[pl.ds(r, 1), :]
                recip_one = recip_ref[0, r]
                if couple:
                    connected_one = right + left.T
                    connected_two = connected_one
                    recip_two = recip_one
                else:
                    connected_one = left + left.T
                    connected_two = right + right.T
                    recip_two = recip_ref[1, r]
                full_one = connected_one + amp * coupling_one
                full_two = connected_two + amp * coupling_two
                total_one = total_one + fold(full_one * full_one * recip_one)
                total_two = total_two + fold(full_two * full_two * recip_two)
            sums_ref[pl.ds(i, 1), :] = jnp.sum(total_one, axis=0, keepdims=True)
            sums_ref[pl.ds(i + occupied, 1), :] = jnp.sum(total_two, axis=0, keepdims=True)
            return carry

        lax.fori_loop(0, occupied, one_occ, 0, unroll=True)

    busy = z < WORKERS

    @pl.when(jnp.logical_and(busy, jnp.logical_not(diagonal)))
    def _():
        both(True)

    @pl.when(jnp.logical_and(busy, diagonal))
    def _():
        both(False)

    energies = jnp.sum(sums_ref[...], axis=1, keepdims=True)
    sub = lax.broadcasted_iota(jnp.int32, (2 * occupied, 128), 0)
    lane = lax.broadcasted_iota(jnp.int32, (2 * occupied, 128), 1)
    block = jnp.where(sub < occupied, info_ref[:, 0:1], info_ref[:, 1:2])
    there = (sub & (occupied - 1)).astype(F32) * 16.0 + block == lane.astype(F32)
    row = jnp.sum(jnp.where(there, energies, 0.0), axis=0, keepdims=True)
    both_rows = jnp.concatenate([row, code_ref[...]], axis=0)
    out_ref[...] = jnp.broadcast_to(both_rows[None], out_ref.shape)


def column_kernel(in_ref, out_ref):
    out_ref[...] = jnp.broadcast_to(jnp.sum(in_ref[...], axis=0, keepdims=True), out_ref.shape)


def final_kernel(in_ref, slots_ref, trip_ref, mean_ref):
    slots = slots_ref.shape[1]
    tables = in_ref[:, 0, :]
    codes = in_ref[:, 1, :] - 1.0
    lane = lax.broadcasted_iota(jnp.int32, codes.shape, 1).astype(F32)
    chosen = jnp.zeros((slots, 128), F32)
    total = jnp.zeros((8, 128), F32)
    columns = [jnp.broadcast_to(codes[:, n:n + 1], codes.shape) - lane for n in range(16)]
    for u in range(4):
        table = tables[u * 8:u * 8 + 8] + tables[(4 + (u ^ 2)) * 8:(4 + (u ^ 2)) * 8 + 8]
        table = jnp.sum(table, axis=0, keepdims=True)
        count = jnp.zeros(codes.shape, F32)
        for column in columns:
            count = count + jnp.where(column == u * 128.0, 1.0, 0.0)
        total = total + jnp.sum(count.reshape(8, 8, 128), axis=0) * table
        chosen = chosen + slots_ref[u] * table
    total = jnp.sum(total, axis=0, keepdims=True)
    mean_ref[...] = jnp.sum(total, axis=1, keepdims=True) / 1024.0
    values = jnp.sum(chosen, axis=1, keepdims=True)
    sub = lax.broadcasted_iota(jnp.int32, (slots, 128), 0)
    lanes = lax.broadcasted_iota(jnp.int32, (slots, 128), 1)
    row = jnp.sum(jnp.where(sub == lanes, values, 0.0), axis=0, keepdims=True)
    trip_ref[...] = row[:, :slots]


def spaces(*kinds):
    return [pl.BlockSpec(memory_space=kind) for kind in kinds]


def vmem(count):
    return spaces(*[pltpu.VMEM] * count)


def kept(*arrays):
    return [pltpu.with_memory_space_constraint(a, pltpu.VMEM) for a in arrays]


def left_in_hbm(*arrays):
    return [pltpu.with_memory_space_constraint(a, pltpu.HBM) for a in arrays]


def rows_call(doubles, coulomb):
    _, width, depth = doubles.shape
    return pl.pallas_call(
        rows_kernel,
        out_shape=pltpu.VMEM((2, width, depth), doubles.dtype),
        in_specs=spaces(pl.ANY, pl.ANY),
        out_specs=vmem(1)[0],
        scratch_shapes=[pltpu.SemaphoreType.DMA((2,))],
        compiler_params=SMALL,
        cost_estimate=pl.CostEstimate(flops=10**9, bytes_accessed=2**20, transcendentals=0),
        name="rows",
    )(*left_in_hbm(doubles, coulomb))


def prep_call(lists, tile_count, occ_energy, vir_energy, singles):
    occupied, width_block = singles.shape
    width = vir_energy.shape[0]
    slots = lists.shape[2]
    return pl.pallas_call(
        prep_kernel,
        out_shape=(
            pltpu.VMEM((2, occupied * width_block, width, width), F32),
            pltpu.VMEM((occupied * width_block, width), F32),
            pltpu.VMEM((1, 128), F32),
            pltpu.VMEM((1, 128), F32),
            pltpu.VMEM((4, slots, 128), F32),
        ),
        in_specs=spaces(*[pltpu.SMEM] * 6, pltpu.VMEM),
        out_specs=tuple(vmem(5)),
        compiler_params=SMALL,
        cost_estimate=pl.CostEstimate(flops=10**10, bytes_accessed=16 * 2**20, transcendentals=2**22),
        name="prep",
    )(*left_in_hbm(jnp.asarray(owner_table()), lists), tile_count, *left_in_hbm(occ_energy, vir_energy, singles, vir_energy[None]))


def energy_call(integrals, one, two, recip, amps, info, code):
    occupied, _, width, _ = integrals.shape
    return pl.pallas_call(
        energy_kernel,
        out_shape=pltpu.VMEM((16, 2, 128), F32),
        in_specs=vmem(7),
        out_specs=vmem(1)[0],
        scratch_shapes=[pltpu.VMEM((2 * occupied, width), F32)],
        compiler_params=SMALL,
        name="energies",
    )(*kept(integrals, one, two, recip, amps, info, code))


def column_call(rows):
    return pl.pallas_call(
        column_kernel,
        out_shape=pltpu.VMEM((64, 2, 128), F32),
        in_specs=vmem(1),
        out_specs=vmem(1)[0],
        compiler_params=SMALL,
        name="column",
    )(*kept(rows))


def final_call(rows, slot_masks):
    slots = slot_masks.shape[1]
    return pl.pallas_call(
        final_kernel,
        out_shape=(jax.ShapeDtypeStruct((1, slots), F32), jax.ShapeDtypeStruct((1, 1), F32)),
        in_specs=vmem(2),
        out_specs=tuple(vmem(2)),
        compiler_params=SMALL,
        name="lookup",
    )(*kept(rows, slot_masks))


def body(integrals, doubles, coulomb, singles, occ_energy, vir_energy, triplets, tile_count):
    near, far = routes()
    sent = rows_call(doubles, coulomb)
    two = lax.ppermute(sent, AXES, far)
    one = lax.ppermute(sent, AXES, near)
    lists = jnp.transpose(triplets, (2, 0, 1))
    recip, amps, info, code, slot_masks = prep_call(lists, tile_count, occ_energy, vir_energy, singles)
    rows = energy_call(integrals, one, two, recip, amps, info, code)
    rows = lax.all_to_all(rows, STACK, 0, 0, tiled=True)
    rows = lax.all_to_all(column_call(rows), PLANE, 0, 0, tiled=True)
    trip, mean = final_call(rows, slot_masks)
    return trip, mean.reshape(())


def solution(mesh):
    fine = Mesh(mesh.devices.reshape(SIZES), AXES)
    in_specs = (
        P(None, BLK, None, None),
        P(BLK, None, None),
        P(BLK, None, None),
        P(None, BLK),
        P(),
        P(),
        P(GRP, None, None),
        P(GRP),
    )
    out_specs = (P(GRP, None), P())
    return jax.shard_map(body, mesh=fine, in_specs=in_specs, out_specs=out_specs, check_vma=False)
```

```python
import jax
import jax.numpy as jnp
import numpy as np
from jax import lax
from jax.experimental import pallas as pl
from jax.experimental.pallas import tpu as pltpu
from jax.sharding import Mesh
from jax.sharding import PartitionSpec as P

AXES = ("yl", "z", "c", "yh", "x")
SIZES = (4, 8, 2, 2, 8)
GRP = ("yl", "z", "c")
BLK = ("yh", "x")
PLANE = ("yh", "yl", "x")
STACK = ("z", "c")
NO = 8
WORKERS = 4
SMALL = pltpu.CompilerParams(vmem_limit_bytes=12 * 1024 * 1024)
F32 = jnp.float32


def device_at(yl, z, c, yh, x):
    return ((((yl * 8) + z) * 2 + c) * 2 + yh) * 8 + x


OWNERS = (
    (0x1739dbf5ace48206, 0x5fd7b193c64e28a0, 0x3961705deaf24b8c, 0xf57d238960c1e4ba,
     0x74b25d310f8cae69, 0x93541706fe2dbac8, 0x0123456789abcdef, 0x6215347098badcfe),
    (0x7f5db1986e4c3a02, 0xf5dc3b1976e420a8, 0x50b317df928e46ca, 0x9475d031ecf2a8b6,
     0x471b5360fa2dce89, 0x89412d05afc3eb67, 0x0132457689abdcef, 0x1324c657089abdfe),
    (0xfb39d5e708a264c1, 0x9ad5bcfe12384706, 0x39ba5d1f8e24c670, 0x138b7fd9204a5c6e,
     0x58a23406f1c9ebd7, 0x21c46370df8ba5e9, 0x70234651a9bcdef8, 0x0241c765ea93bd8f),
    (0x73b91efdc20864a5, 0xdb679fc30a1e8542, 0xf97a6d15b324e8c0, 0x589b73d120a64fec,
     0x0152364f89bcaed7, 0x3210b7549ecaf68d, 0x10234567a89bcdfe, 0x2a315470eb89dc6f),
)
APART = 2


def owner_table():
    digits = [[[int(d, 16) for d in f"{code:016x}"] for code in codes] for codes in OWNERS]
    return np.array(digits, np.int32).reshape(-1)


def owner_index(yl, z, c, yh, x):
    return (((yl ^ (2 * yh)) * WORKERS + z % WORKERS) * 2 + c) * 16 + yh * 8 + x


def pairs_of(owner, u, where):
    swapped = ((owner & 1) << 3) | ((owner & 6) ^ (u << 1)) | (owner >> 3)
    other = where(swapped == owner, owner ^ APART, swapped)
    return other, pair_at(owner, u), pair_at(other, u)


def pair_at(owner, u):
    return owner >> 1, (owner & 1) * 4 + (((owner >> 1) & 3) ^ u)


def routes():
    table, near, far = owner_table(), [], []
    for yl, z, c, yh, x in np.ndindex(*SIZES):
        if z < WORKERS:
            here, u = device_at(yl, z, c, yh, x), yl ^ (2 * yh)
            owner = int(table[owner_index(yl, z, c, yh, x)])
            other, _, _ = pairs_of(owner, u, lambda a, b, c: b if a else c)
            for route, block in ((near, owner), (far, other)):
                half = block >> 3
                route.append((device_at(u ^ (2 * half), z, c, half, block & 7), here))
    return near, far


def where_am_i():
    yl, z, c, yh, x = (lax.axis_index(axis) for axis in AXES)
    return yl, z, c, yh, x


def rows_kernel(doubles_ref, coulomb_ref, out_ref, sems):
    yl, z, _, yh, x = where_am_i()
    row = (((yh * 8 + x) >> 1) & 3) ^ yl ^ (2 * yh)
    copies = [
        pltpu.make_async_copy(doubles_ref.at[row], out_ref.at[0], sems.at[0]),
        pltpu.make_async_copy(coulomb_ref.at[row], out_ref.at[1], sems.at[1]),
    ]

    @pl.when(z < WORKERS)
    def _():
        for copy in copies:
            copy.start()
        for copy in copies:
            copy.wait()


def prep_kernel(owners_ref, trip_ref, count_ref, occ_ref, vir_ref, singles_ref, virs_ref,
                recip_ref, amps_ref, info_ref, code_ref, slots_ref):
    occupied, width_block = singles_ref.shape
    width = virs_ref.shape[1]
    slots = trip_ref.shape[2]
    yl, z, c, yh, x = where_am_i()
    place = yh * 8 + x
    owner = owners_ref[owner_index(yl, z, c, yh, x)]
    other, (j1, k1), (j2, k2) = pairs_of(owner, yl ^ (2 * yh), jnp.where)
    diagonal = j1 == k1
    busy = z < WORKERS
    live = count_ref[0]

    lane = lax.broadcasted_iota(jnp.int32, (1, 128), 1)
    info = jnp.where(lane == 0, owner.astype(F32), 0.0)
    info = jnp.where(lane == 1, other.astype(F32), info)
    info_ref[...] = jnp.where(lane == 2, diagonal.astype(F32), info)

    def code_of(s):
        i, j, k = trip_ref[0, 0, s], trip_ref[1, 0, s], trip_ref[2, 0, s]
        code = ((j ^ k) & 3) * 128 + i * 16 + j * 2 + (k >> 2)
        return jnp.where(s < live, code, -1)

    code_ref[...] = jnp.where(lane == z * 2 + c, (code_of(place) + 1).astype(F32), 0.0)

    sub = lax.broadcasted_iota(jnp.int32, (slots, 128), 0)
    lanes = lax.broadcasted_iota(jnp.int32, (slots, 128), 1)
    codes = jnp.full((slots, 128), -1, jnp.int32)
    for s in range(slots):
        codes = jnp.where(sub == s, code_of(s), codes)
    for u in range(4):
        slots_ref[u] = jnp.where(codes == u * 128 + lanes, 1.0, 0.0)

    def fill(table, second, third, write_amps):
        across = jnp.broadcast_to(virs_ref[...], (width, width))
        sums = across.T + across

        def one_occ(i, carry):
            occ_sum = occ_ref[i] + occ_ref[second] + occ_ref[third]
            for a in range(width_block):
                r = i * width_block + a
                recip_ref[table, r] = 1.0 / ((occ_sum - vir_ref[place * width_block + a]) - sums)
                if write_amps:
                    amps_ref[pl.ds(r, 1), :] = jnp.full((1, 128), singles_ref[i, a], F32)
            return carry

        lax.fori_loop(0, occupied, one_occ, 0)

    @pl.when(busy)
    def _():
        fill(0, j1, k1, True)

    @pl.when(jnp.logical_and(busy, diagonal))
    def _():
        fill(1, j2, k2, False)


def energy_kernel(ints_ref, one_ref, two_ref, recip_ref, amps_ref, info_ref, code_ref, out_ref, sums_ref):
    occupied, width_block, width, _ = ints_ref.shape
    _, z, _, _, _ = where_am_i()
    diagonal = jnp.max(info_ref[:, 2:3]) > 0.5
    sums_ref[...] = jnp.zeros(sums_ref.shape, F32)

    def fold(value):
        return jnp.sum(value.reshape(width // 8, 8, width), axis=0)

    def both(couple):
        amps = jnp.concatenate([one_ref[0], two_ref[0]], axis=0)
        coupling_one = one_ref[1].astype(F32)
        coupling_two = two_ref[1].astype(F32)
        if couple:
            coupling_two = coupling_two.T

        def one_occ(i, carry):
            slab = ints_ref[i].reshape(width_block * width, width)
            products = lax.dot_general(slab, amps, (((1,), (1,)), ((), ())), preferred_element_type=F32)
            total_one = jnp.zeros((8, width), F32)
            total_two = jnp.zeros((8, width), F32)
            for a in range(width_block):
                r = i * width_block + a
                left = products[a * width:(a + 1) * width, :width]
                right = products[a * width:(a + 1) * width, width:]
                amp = amps_ref[pl.ds(r, 1), :]
                recip_one = recip_ref[0, r]
                if couple:
                    connected_one = right + left.T
                    connected_two = connected_one
                    recip_two = recip_one
                else:
                    connected_one = left + left.T
                    connected_two = right + right.T
                    recip_two = recip_ref[1, r]
                full_one = connected_one + amp * coupling_one
                full_two = connected_two + amp * coupling_two
                total_one = total_one + fold(full_one * full_one * recip_one)
                total_two = total_two + fold(full_two * full_two * recip_two)
            sums_ref[pl.ds(i, 1), :] = jnp.sum(total_one, axis=0, keepdims=True)
            sums_ref[pl.ds(i + occupied, 1), :] = jnp.sum(total_two, axis=0, keepdims=True)
            return carry

        lax.fori_loop(0, occupied, one_occ, 0, unroll=True)

    busy = z < WORKERS

    @pl.when(jnp.logical_and(busy, jnp.logical_not(diagonal)))
    def _():
        both(True)

    @pl.when(jnp.logical_and(busy, diagonal))
    def _():
        both(False)

    energies = jnp.sum(sums_ref[...], axis=1, keepdims=True)
    sub = lax.broadcasted_iota(jnp.int32, (2 * occupied, 128), 0)
    lane = lax.broadcasted_iota(jnp.int32, (2 * occupied, 128), 1)
    block = jnp.where(sub < occupied, info_ref[:, 0:1], info_ref[:, 1:2])
    there = (sub & (occupied - 1)).astype(F32) * 16.0 + block == lane.astype(F32)
    row = jnp.sum(jnp.where(there, energies, 0.0), axis=0, keepdims=True)
    even = lax.broadcasted_iota(jnp.int32, out_ref.shape, 0) % 2 == 0
    out_ref[...] = jnp.where(even, row, code_ref[...])


def column_kernel(in_ref, out_ref):
    total = jnp.sum(in_ref[...].reshape(4, 8, 128), axis=0)
    total = total + pltpu.roll(total, 4, 0)
    total = total + pltpu.roll(total, 2, 0)
    out_ref[...] = jnp.broadcast_to(total[None], (16, 8, 128)).reshape(128, 128)


def final_kernel(in_ref, slots_ref, trip_ref, mean_ref):
    slots = slots_ref.shape[1]
    lane = lax.broadcasted_iota(jnp.int32, (8, 128), 1).astype(F32) + 1.0
    counts = [jnp.zeros((8, 128), F32) for _ in range(4)]
    tables = []
    for q in range(8):
        tables.append(in_ref[pl.ds(16 * q, 8, 2), :])
        codes = in_ref[pl.ds(16 * q + 1, 8, 2), :]
        for n in range(16):
            column = jnp.broadcast_to(codes[:, n:n + 1], (8, 128)) - lane
            for u in range(4):
                counts[u] = counts[u] + jnp.where(column == u * 128.0, 1.0, 0.0)
    chosen = jnp.zeros((slots, 128), F32)
    total = jnp.zeros((8, 128), F32)
    for u in range(4):
        table = jnp.sum(tables[u] + tables[4 + (u ^ 2)], axis=0, keepdims=True)
        total = total + counts[u] * table
        chosen = chosen + slots_ref[u] * table
    total = jnp.sum(total, axis=0, keepdims=True)
    mean_ref[...] = jnp.sum(total, axis=1, keepdims=True) / 1024.0
    values = jnp.sum(chosen, axis=1, keepdims=True)
    sub = lax.broadcasted_iota(jnp.int32, (slots, 128), 0)
    lanes = lax.broadcasted_iota(jnp.int32, (slots, 128), 1)
    row = jnp.sum(jnp.where(sub == lanes, values, 0.0), axis=0, keepdims=True)
    trip_ref[...] = row[:, :slots]


def spaces(*kinds):
    return [pl.BlockSpec(memory_space=kind) for kind in kinds]


def vmem(count):
    return spaces(*[pltpu.VMEM] * count)


def kept(*arrays):
    return [pltpu.with_memory_space_constraint(a, pltpu.VMEM) for a in arrays]


def left_in_hbm(*arrays):
    return [pltpu.with_memory_space_constraint(a, pltpu.HBM) for a in arrays]


def rows_call(doubles, coulomb):
    _, width, depth = doubles.shape
    return pl.pallas_call(
        rows_kernel,
        out_shape=pltpu.VMEM((2, width, depth), doubles.dtype),
        in_specs=spaces(pl.ANY, pl.ANY),
        out_specs=vmem(1)[0],
        scratch_shapes=[pltpu.SemaphoreType.DMA((2,))],
        compiler_params=SMALL,
        cost_estimate=pl.CostEstimate(flops=10**9, bytes_accessed=2**20, transcendentals=0),
        name="rows",
    )(*left_in_hbm(doubles, coulomb))


def prep_call(lists, tile_count, occ_energy, vir_energy, singles):
    occupied, width_block = singles.shape
    width = vir_energy.shape[0]
    slots = lists.shape[2]
    return pl.pallas_call(
        prep_kernel,
        out_shape=(
            pltpu.VMEM((2, occupied * width_block, width, width), F32),
            pltpu.VMEM((occupied * width_block, width), F32),
            pltpu.VMEM((1, 128), F32),
            pltpu.VMEM((1, 128), F32),
            pltpu.VMEM((4, slots, 128), F32),
        ),
        in_specs=spaces(*[pltpu.SMEM] * 6, pltpu.VMEM),
        out_specs=tuple(vmem(5)),
        compiler_params=SMALL,
        cost_estimate=pl.CostEstimate(flops=10**10, bytes_accessed=16 * 2**20, transcendentals=2**22),
        name="prep",
    )(*left_in_hbm(jnp.asarray(owner_table()), lists), tile_count, *left_in_hbm(occ_energy, vir_energy, singles, vir_energy[None]))


def energy_call(integrals, one, two, recip, amps, info, code):
    occupied, _, width, _ = integrals.shape
    return pl.pallas_call(
        energy_kernel,
        out_shape=pltpu.VMEM((32, 128), F32),
        in_specs=vmem(7),
        out_specs=vmem(1)[0],
        scratch_shapes=[pltpu.VMEM((2 * occupied, width), F32)],
        compiler_params=SMALL,
        name="energies",
    )(*kept(integrals, one, two, recip, amps, info, code))


def column_call(rows):
    return pl.pallas_call(
        column_kernel,
        out_shape=pltpu.VMEM((128, 128), F32),
        in_specs=vmem(1),
        out_specs=vmem(1)[0],
        compiler_params=SMALL,
        name="column",
    )(*kept(rows))


def final_call(rows, slot_masks):
    slots = slot_masks.shape[1]
    return pl.pallas_call(
        final_kernel,
        out_shape=(jax.ShapeDtypeStruct((1, slots), F32), jax.ShapeDtypeStruct((1, 1), F32)),
        in_specs=vmem(2),
        out_specs=tuple(vmem(2)),
        compiler_params=SMALL,
        name="lookup",
    )(*kept(rows, slot_masks))


def body(integrals, doubles, coulomb, singles, occ_energy, vir_energy, triplets, tile_count):
    near, far = routes()
    sent = rows_call(doubles, coulomb)
    two = lax.ppermute(sent, AXES, far)
    one = lax.ppermute(sent, AXES, near)
    lists = jnp.transpose(triplets, (2, 0, 1))
    recip, amps, info, code, slot_masks = prep_call(lists, tile_count, occ_energy, vir_energy, singles)
    rows = energy_call(integrals, one, two, recip, amps, info, code)
    rows = lax.all_to_all(rows, STACK, 0, 0, tiled=True)
    rows = lax.all_to_all(column_call(rows), PLANE, 0, 0, tiled=True)
    trip, mean = final_call(rows, slot_masks)
    return trip, mean.reshape(())


def solution(mesh):
    fine = Mesh(mesh.devices.reshape(SIZES), AXES)
    in_specs = (
        P(None, BLK, None, None),
        P(BLK, None, None),
        P(BLK, None, None),
        P(None, BLK),
        P(),
        P(),
        P(GRP, None, None),
        P(GRP),
    )
    out_specs = (P(GRP, None), P())
    return jax.shard_map(body, mesh=fine, in_specs=in_specs, out_specs=out_specs, check_vma=False)
```

```python
import jax
import jax.numpy as jnp
import numpy as np
from jax import lax
from jax.experimental import pallas as pl
from jax.experimental.pallas import tpu as pltpu
from jax.sharding import Mesh
from jax.sharding import PartitionSpec as P

AXES = ("yl", "z", "c", "yh", "x")
SIZES = (4, 8, 2, 2, 8)
GRP = ("yl", "z", "c")
BLK = ("yh", "x")
PLANE = ("yh", "yl", "x")
STACK = ("z", "c")
NO = 8
WORKERS = 4
SMALL = pltpu.CompilerParams(vmem_limit_bytes=12 * 1024 * 1024)
F32 = jnp.float32


def device_at(yl, z, c, yh, x):
    return ((((yl * 8) + z) * 2 + c) * 2 + yh) * 8 + x


OWNERS = (
    (0x1975dbf3ec0284a6, 0xf58db139c7e4620a, 0xeb947d1562c8a3f0, 0x5ab713df902e486c,
     0x20315476af9bdc8e, 0x365b27410a8defc9, 0x01234567f9bacde8, 0x9742365081acbedf),
    (0xf5bda1897c4e3602, 0x7fdc3b9856e420a1, 0x5943b7f160d2eac8, 0x9475d21f0e3ca8b6,
     0x401b2d56fa93ce87, 0x8751c30eaf2d4b69, 0x0132456789cabdef, 0x1324567098abdcfe),
    (0x39ba7df1e2485c60, 0x1f395b7d8ea0264c, 0x9751b3df602ac48e, 0xf59bdc1e08324a76,
     0x23a4c608f19be5d7, 0x024537e61f89abcd, 0x71234560a9bcdef8, 0x801264579ac3bdef),
    (0x3b791efd20c8645a, 0xb5179fd3ca068e42, 0xa2917d35fcb4e860, 0xf7b0d354a21e968c,
     0x790b364fd12ca5e8, 0x23a567e10b894fcd, 0x1023456789abcdfe, 0x01325476e89abcdf),
)
APART = 4


def owner_table():
    digits = [[[int(d, 16) for d in f"{code:016x}"] for code in codes] for codes in OWNERS]
    return np.array(digits, np.int32).reshape(-1)


def owner_index(yl, z, c, yh, x):
    return (((yl ^ (2 * yh)) * WORKERS + z % WORKERS) * 2 + c) * 16 + yh * 8 + x


def pairs_of(owner, u, where):
    swapped = ((owner & 1) << 3) | ((owner & 6) ^ (u << 1)) | (owner >> 3)
    other = where(swapped == owner, owner ^ APART, swapped)
    return other, pair_at(owner, u), pair_at(other, u)


def pair_at(owner, u):
    return owner >> 1, (owner & 1) * 4 + (((owner >> 1) & 3) ^ u)


def routes():
    table, near, far = owner_table(), [], []
    for yl, z, c, yh, x in np.ndindex(*SIZES):
        if z < WORKERS:
            here, u = device_at(yl, z, c, yh, x), yl ^ (2 * yh)
            owner = int(table[owner_index(yl, z, c, yh, x)])
            other, _, _ = pairs_of(owner, u, lambda a, b, c: b if a else c)
            for route, block in ((near, owner), (far, other)):
                half = block >> 3
                route.append((device_at(u ^ (2 * half), z, c, half, block & 7), here))
    return near, far


def where_am_i():
    yl, z, c, yh, x = (lax.axis_index(axis) for axis in AXES)
    return yl, z, c, yh, x


def rows_kernel(doubles_ref, coulomb_ref, out_ref, sems):
    yl, z, _, yh, x = where_am_i()
    row = (((yh * 8 + x) >> 1) & 3) ^ yl ^ (2 * yh)
    copies = [
        pltpu.make_async_copy(doubles_ref.at[row], out_ref.at[0], sems.at[0]),
        pltpu.make_async_copy(coulomb_ref.at[row], out_ref.at[1], sems.at[1]),
    ]

    @pl.when(z < WORKERS)
    def _():
        for copy in copies:
            copy.start()
        for copy in copies:
            copy.wait()


def prep_kernel(owners_ref, trip_ref, count_ref, occ_ref, vir_ref, singles_ref, virs_ref,
                recip_ref, amps_ref, info_ref, code_ref, slots_ref):
    occupied, width_block = singles_ref.shape
    width = virs_ref.shape[1]
    slots = trip_ref.shape[2]
    yl, z, c, yh, x = where_am_i()
    place = yh * 8 + x
    owner = owners_ref[owner_index(yl, z, c, yh, x)]
    other, (j1, k1), (j2, k2) = pairs_of(owner, yl ^ (2 * yh), jnp.where)
    diagonal = j1 == k1
    busy = z < WORKERS
    live = count_ref[0]

    lane = lax.broadcasted_iota(jnp.int32, (1, 128), 1)
    info = jnp.where(lane == 0, owner.astype(F32), 0.0)
    info = jnp.where(lane == 1, other.astype(F32), info)
    info_ref[...] = jnp.where(lane == 2, diagonal.astype(F32), info)

    def code_of(s):
        i, j, k = trip_ref[0, 0, s], trip_ref[1, 0, s], trip_ref[2, 0, s]
        code = ((j ^ k) & 3) * 128 + i * 16 + j * 2 + (k >> 2)
        return jnp.where(s < live, code, -1)

    code_ref[...] = jnp.where(lane == z * 2 + c, (code_of(place) + 1).astype(F32), 0.0)

    sub = lax.broadcasted_iota(jnp.int32, (slots, 128), 0)
    lanes = lax.broadcasted_iota(jnp.int32, (slots, 128), 1)
    codes = jnp.full((slots, 128), -1, jnp.int32)
    for s in range(slots):
        codes = jnp.where(sub == s, code_of(s), codes)
    for u in range(4):
        slots_ref[u] = jnp.where(codes == u * 128 + lanes, 1.0, 0.0)

    def fill(table, second, third, write_amps):
        across = jnp.broadcast_to(virs_ref[...], (width, width))
        sums = across.T + across

        def one_occ(i, carry):
            occ_sum = occ_ref[i] + occ_ref[second] + occ_ref[third]
            for a in range(width_block):
                r = i * width_block + a
                recip_ref[table, r] = 1.0 / ((occ_sum - vir_ref[place * width_block + a]) - sums)
                if write_amps:
                    amps_ref[pl.ds(r, 1), :] = jnp.full((1, 128), singles_ref[i, a], F32)
            return carry

        lax.fori_loop(0, occupied, one_occ, 0)

    @pl.when(busy)
    def _():
        fill(0, j1, k1, True)

    @pl.when(jnp.logical_and(busy, diagonal))
    def _():
        fill(1, j2, k2, False)


def energy_kernel(ints_ref, one_ref, two_ref, recip_ref, amps_ref, info_ref, code_ref, out_ref, sums_ref):
    occupied, width_block, width, _ = ints_ref.shape
    _, z, _, _, _ = where_am_i()
    diagonal = jnp.max(info_ref[:, 2:3]) > 0.5
    sums_ref[...] = jnp.zeros(sums_ref.shape, F32)

    def fold(value):
        return jnp.sum(value.reshape(width // 8, 8, width), axis=0)

    def both(couple):
        amps = jnp.concatenate([one_ref[0], two_ref[0]], axis=0)
        coupling_one = one_ref[1].astype(F32)
        coupling_two = two_ref[1].astype(F32)
        if couple:
            coupling_two = coupling_two.T

        def one_occ(i, carry):
            slab = ints_ref[i].reshape(width_block * width, width)
            products = lax.dot_general(slab, amps, (((1,), (1,)), ((), ())), preferred_element_type=F32)
            total_one = jnp.zeros((8, width), F32)
            total_two = jnp.zeros((8, width), F32)
            for a in range(width_block):
                r = i * width_block + a
                left = products[a * width:(a + 1) * width, :width]
                right = products[a * width:(a + 1) * width, width:]
                amp = amps_ref[pl.ds(r, 1), :]
                recip_one = recip_ref[0, r]
                if couple:
                    connected_one = right + left.T
                    connected_two = connected_one
                    recip_two = recip_one
                else:
                    connected_one = left + left.T
                    connected_two = right + right.T
                    recip_two = recip_ref[1, r]
                full_one = connected_one + amp * coupling_one
                full_two = connected_two + amp * coupling_two
                total_one = total_one + fold(full_one * full_one * recip_one)
                total_two = total_two + fold(full_two * full_two * recip_two)
            sums_ref[pl.ds(i, 1), :] = jnp.sum(total_one, axis=0, keepdims=True)
            sums_ref[pl.ds(i + occupied, 1), :] = jnp.sum(total_two, axis=0, keepdims=True)
            return carry

        lax.fori_loop(0, occupied, one_occ, 0, unroll=True)

    busy = z < WORKERS

    @pl.when(jnp.logical_and(busy, jnp.logical_not(diagonal)))
    def _():
        both(True)

    @pl.when(jnp.logical_and(busy, diagonal))
    def _():
        both(False)

    energies = jnp.sum(sums_ref[...], axis=1, keepdims=True)
    sub = lax.broadcasted_iota(jnp.int32, (2 * occupied, 128), 0)
    lane = lax.broadcasted_iota(jnp.int32, (2 * occupied, 128), 1)
    block = jnp.where(sub < occupied, info_ref[:, 0:1], info_ref[:, 1:2])
    there = (sub & (occupied - 1)).astype(F32) * 16.0 + block == lane.astype(F32)
    row = jnp.sum(jnp.where(there, energies, 0.0), axis=0, keepdims=True)
    even = lax.broadcasted_iota(jnp.int32, out_ref.shape, 0) % 2 == 0
    out_ref[...] = jnp.where(even, row, code_ref[...])


def column_kernel(in_ref, out_ref):
    total = jnp.sum(in_ref[...].reshape(4, 8, 128), axis=0)
    total = total + pltpu.roll(total, 4, 0)
    total = total + pltpu.roll(total, 2, 0)
    out_ref[...] = jnp.broadcast_to(total[None], (16, 8, 128)).reshape(128, 128)


def final_kernel(in_ref, slots_ref, trip_ref, mean_ref):
    slots = slots_ref.shape[1]
    lane = lax.broadcasted_iota(jnp.int32, (8, 128), 1).astype(F32) + 1.0
    counts = [jnp.zeros((8, 128), F32) for _ in range(4)]
    tables = []
    for q in range(8):
        tables.append(in_ref[pl.ds(16 * q, 8, 2), :])
        codes = in_ref[pl.ds(16 * q + 1, 8, 2), :]
        for n in range(16):
            column = jnp.broadcast_to(codes[:, n:n + 1], (8, 128)) - lane
            for u in range(4):
                counts[u] = counts[u] + jnp.where(column == u * 128.0, 1.0, 0.0)
    chosen = jnp.zeros((slots, 128), F32)
    total = jnp.zeros((8, 128), F32)
    for u in range(4):
        table = jnp.sum(tables[u] + tables[4 + (u ^ 2)], axis=0, keepdims=True)
        total = total + counts[u] * table
        chosen = chosen + slots_ref[u] * table
    total = jnp.sum(total, axis=0, keepdims=True)
    mean_ref[...] = jnp.sum(total, axis=1, keepdims=True) / 1024.0
    values = jnp.sum(chosen, axis=1, keepdims=True)
    sub = lax.broadcasted_iota(jnp.int32, (slots, 128), 0)
    lanes = lax.broadcasted_iota(jnp.int32, (slots, 128), 1)
    row = jnp.sum(jnp.where(sub == lanes, values, 0.0), axis=0, keepdims=True)
    trip_ref[...] = row[:, :slots]


def spaces(*kinds):
    return [pl.BlockSpec(memory_space=kind) for kind in kinds]


def vmem(count):
    return spaces(*[pltpu.VMEM] * count)


def kept(*arrays):
    return [pltpu.with_memory_space_constraint(a, pltpu.VMEM) for a in arrays]


def left_in_hbm(*arrays):
    return [pltpu.with_memory_space_constraint(a, pltpu.HBM) for a in arrays]


def rows_call(doubles, coulomb):
    _, width, depth = doubles.shape
    return pl.pallas_call(
        rows_kernel,
        out_shape=pltpu.VMEM((2, width, depth), doubles.dtype),
        in_specs=spaces(pl.ANY, pl.ANY),
        out_specs=vmem(1)[0],
        scratch_shapes=[pltpu.SemaphoreType.DMA((2,))],
        compiler_params=SMALL,
        cost_estimate=pl.CostEstimate(flops=10**9, bytes_accessed=2**20, transcendentals=0),
        name="rows",
    )(*left_in_hbm(doubles, coulomb))


def prep_call(lists, tile_count, occ_energy, vir_energy, singles):
    occupied, width_block = singles.shape
    width = vir_energy.shape[0]
    slots = lists.shape[2]
    return pl.pallas_call(
        prep_kernel,
        out_shape=(
            pltpu.VMEM((2, occupied * width_block, width, width), F32),
            pltpu.VMEM((occupied * width_block, width), F32),
            pltpu.VMEM((1, 128), F32),
            pltpu.VMEM((1, 128), F32),
            pltpu.VMEM((4, slots, 128), F32),
        ),
        in_specs=spaces(*[pltpu.SMEM] * 6, pltpu.VMEM),
        out_specs=tuple(vmem(5)),
        compiler_params=SMALL,
        cost_estimate=pl.CostEstimate(flops=10**10, bytes_accessed=16 * 2**20, transcendentals=2**22),
        name="prep",
    )(*left_in_hbm(jnp.asarray(owner_table()), lists), tile_count, *left_in_hbm(occ_energy, vir_energy, singles, vir_energy[None]))


def energy_call(integrals, one, two, recip, amps, info, code):
    occupied, _, width, _ = integrals.shape
    return pl.pallas_call(
        energy_kernel,
        out_shape=pltpu.VMEM((32, 128), F32),
        in_specs=vmem(7),
        out_specs=vmem(1)[0],
        scratch_shapes=[pltpu.VMEM((2 * occupied, width), F32)],
        compiler_params=SMALL,
        name="energies",
    )(*kept(integrals, one, two, recip, amps, info, code))


def column_call(rows):
    return pl.pallas_call(
        column_kernel,
        out_shape=pltpu.VMEM((128, 128), F32),
        in_specs=vmem(1),
        out_specs=vmem(1)[0],
        compiler_params=SMALL,
        name="column",
    )(*kept(rows))


def final_call(rows, slot_masks):
    slots = slot_masks.shape[1]
    return pl.pallas_call(
        final_kernel,
        out_shape=(jax.ShapeDtypeStruct((1, slots), F32), jax.ShapeDtypeStruct((1, 1), F32)),
        in_specs=vmem(2),
        out_specs=tuple(vmem(2)),
        compiler_params=SMALL,
        name="lookup",
    )(*kept(rows, slot_masks))


def body(integrals, doubles, coulomb, singles, occ_energy, vir_energy, triplets, tile_count):
    near, far = routes()
    sent = rows_call(doubles, coulomb)
    two = lax.ppermute(sent, AXES, far)
    one = lax.ppermute(sent, AXES, near)
    lists = jnp.transpose(triplets, (2, 0, 1))
    recip, amps, info, code, slot_masks = prep_call(lists, tile_count, occ_energy, vir_energy, singles)
    rows = energy_call(integrals, one, two, recip, amps, info, code)
    rows = lax.all_to_all(rows, STACK, 0, 0, tiled=True)
    rows = lax.all_to_all(column_call(rows), PLANE, 0, 0, tiled=True)
    trip, mean = final_call(rows, slot_masks)
    return trip, mean.reshape(())


def solution(mesh):
    fine = Mesh(mesh.devices.reshape(SIZES), AXES)
    in_specs = (
        P(None, BLK, None, None),
        P(BLK, None, None),
        P(BLK, None, None),
        P(None, BLK),
        P(),
        P(),
        P(GRP, None, None),
        P(GRP),
    )
    out_specs = (P(GRP, None), P())
    return jax.shard_map(body, mesh=fine, in_specs=in_specs, out_specs=out_specs, check_vma=False)
```
